32 devices in a mesh: clip: 2 (over y), patch: 4 (over z), head: 2 (over x), rep: 2 (over core).
Axes of the slice: x: 2, y: 2, z: 4, core: 2. Of those that a mesh axis runs over, the one named last changes fastest.
Arguments:
- tokens: bfloat16 [1024, 3072], P(('clip', 'patch', 'head', 'rep')), parts along dimension 0, may hold values from -24 to 24
- modulation: float32 [3, 3072], replicated, may hold values from -3 to 3
- in_weight: bfloat16 [3072, 16, 384], P(None, ('head', 'rep')), may hold values from -0.109375 to 0.109375
- query_gain: float32 [128], replicated, may hold values from 1 to 2.5
- key_gain: float32 [128], replicated, may hold values from 0.25 to 1.75
- out_weight: bfloat16 [16, 128, 3072], P(('head', 'rep')), may hold values from -1.5 to 1.5
- stale_cache: bfloat16 [1024, 16, 256], P(('clip', 'patch', 'head', 'rep')), parts along dimension 0, may hold values from -440 to 440, as said below
- lengths: int32 [8], P('clip'), parts along dimension 0, may hold values from 1 to 128, 384 in all
Outputs:
- update: bfloat16 [1024, 3072], P(('clip', 'patch', 'head', 'rep')), parts along dimension 0
- new_cache: bfloat16 [1024, 16, 256], P(('clip', 'patch', 'head', 'rep')), parts along dimension 0
The draws below stay inside these ranges and needn't reach their ends.
There are 2 independent parts, one for each index of `clip`. The reference program is written for one: setup_inputs(seed, part) draws one part's arguments, and reference() takes and returns one part's arrays. A program takes and returns all parts, laid end to end along the dimension named above; an argument that names none is the same for every part. Nothing has to cross between parts.
Inputs may be any that keep to these rules, and one draw needn't show every extreme that they name: stale_cache[s, h] holds the stale key of token s and head h in its first 128 entries and the stale value in its last 128. Only the first lengths[p] tokens of patch p are live keys.
All inputs are finite; a program needn't handle non-finite values.
Results may differ from the reference program's by a relative error of at most 0.02.
The reference program's roundings to bfloat16 on the way count: a program that leaves them out, or rounds other values in their place, can miss the bound.
Values may be sent and summed in bfloat16 or wider, within the bound.
A program may use at most 128 MiB of HBM per device.

```python
import math
import jax
import jax.numpy as jnp
import numpy as np
from jax import lax

D = 3072
HD = 128
H = 16
HEAD_GROUPS = 4
PATCH_TOK = 128
SEQ = 512
LIVE = 384
N_PATCH = 4


def draw_tokens(key, part):
    key_rows, key_columns, key_entries = jax.random.split(key, 3)
    row_scale = jnp.exp(jax.random.uniform(key_rows, (SEQ, 1), jnp.float32, math.log(0.3), math.log(3.0)))
    column_scale = jnp.exp(jax.random.uniform(key_columns, (1, D), jnp.float32, math.log(0.3), math.log(3.0)))
    entries = jax.random.normal(key_entries, (SEQ, D), jnp.float32)
    values = entries * column_scale * row_scale
    return jnp.clip(values, -24.0, 24.0).astype(jnp.bfloat16)


def draw_stale_cache(key, part):
    key_entries = jax.random.fold_in(key, 0)
    array_shape = (SEQ, H, 2 * HD)
    entries = jax.random.normal(key_entries, array_shape, jnp.float32)
    return jnp.clip(entries, -6.0, 6.0).astype(jnp.bfloat16)


def shard_levels(own_key, extent, cuts, least, largest):
    factor_of, own = 1.0, jax.random.fold_in(own_key, 6)
    for dim, shards_of in cuts:
        steps = jnp.exp(jax.random.uniform(jax.random.fold_in(own, dim), (shards_of,), jnp.float32, least / len(cuts), largest / len(cuts)))
        factor_of = factor_of * jnp.repeat(steps, extent[dim] // shards_of).reshape([-1 if axis == dim else 1 for axis in range(len(extent))])
    return factor_of


def length_profile(amount, total, reach, skew):
    weights = [(1 << 20) // math.isqrt(rank ** skew) + 1 for rank in range(2, amount + 1)]
    surplus, holding = total - reach - (amount - 1), [1] * (amount - 1)
    while surplus > 0:
        movable = [i for i in range(amount - 1) if holding[i] < reach]
        mass, left = sum([weights[i] for i in movable]), surplus
        for i in movable:
            more = min(reach - holding[i], max(1, left * weights[i] // mass), surplus)
            holding[i] = holding[i] + more
            surplus = surplus - more
    return np.array([reach] + holding)


def uneven(stream_key, amount, total, limit, slope):
    if amount == 2:
        one = jax.random.randint(stream_key, (), max(1, total - limit), min(limit, total - 1) + 1)
        return jnp.stack([one, total - one])
    tallies = jnp.asarray(length_profile(amount, total, limit, slope), jnp.int32)
    pairs = (amount - 1) // 2
    source_of, taker = tallies[1:1 + 2 * pairs:2], tallies[2:2 + 2 * pairs:2]
    slack = jnp.minimum(source_of - 1, limit - taker)
    moved = jax.random.randint(jax.random.fold_in(stream_key, 1), (pairs,), 0, 1 << 20) % (slack + 1)
    tallies = tallies.at[1:1 + 2 * pairs:2].set(source_of - moved).at[2:2 + 2 * pairs:2].set(taker + moved)
    return tallies[jax.random.permutation(jax.random.fold_in(stream_key, 2), amount)]


def normal_values(rng, dims, spread, bound, shards=(), held_as=jnp.bfloat16):
    values = spread * jax.random.normal(rng, dims, jnp.float32)
    if shards:
        values = values * shard_levels(rng, dims, shards, -0.22, 0.18)
    return jnp.clip(values, -bound, bound).astype(held_as)


def setup_inputs(seed: int = 0, part: int = 0) -> dict:
    key_of = jax.random.split(jax.random.key(seed), 9)
    part_splits = jax.random.split(jax.random.fold_in(key_of[8], part), 9)
    tokens = draw_tokens(jax.random.fold_in(jax.random.fold_in(key_of[8], part), 71), part)
    modulation = normal_values(key_of[1], (3, D), 0.5, 3.0, (), jnp.float32)
    in_weight = normal_values(key_of[2], (D, H, 3 * HD), D ** -0.5, 0.109375, ((1, 4),))
    query_gain = jnp.clip(jnp.exp(jax.random.uniform(key_of[3], (HD,), jnp.float32, math.log(1.0), math.log(2.5))), 1.0, 2.5)
    key_gain = jnp.clip(1.0 + 0.15 * jax.random.normal(key_of[4], (HD,), jnp.float32), 0.25, 1.75)
    out_weight = normal_values(key_of[5], (H, HD, D), 0.25, 1.5, ((0, 4),))
    stale_cache = draw_stale_cache(jax.random.fold_in(jax.random.fold_in(key_of[8], part), 71), part)
    lengths = uneven(part_splits[7], N_PATCH, LIVE, PATCH_TOK, 1).astype(jnp.int32)
    return dict(tokens=tokens, modulation=modulation, in_weight=in_weight, query_gain=query_gain, key_gain=key_gain, out_weight=out_weight, stale_cache=stale_cache, lengths=lengths)


EPSILON = 1e-06
NEGATIVE = -1e+30

def normalize_rows(values):
    average = lax.optimization_barrier(jnp.mean(values, axis=-1, keepdims=True))
    centred = values - average
    variance = lax.optimization_barrier(jnp.mean(centred * centred, axis=-1, keepdims=True))
    return centred * lax.rsqrt(variance + EPSILON)

def rms_gain(values, gain):
    return values * lax.rsqrt(lax.optimization_barrier(jnp.mean(values * values, axis=-1, keepdims=True)) + EPSILON) * gain

def project(normed, in_weight, query_gain, key_gain):
    row_count = normed.shape[0]
    head_count = in_weight.shape[1]
    triple = in_weight.shape[2]
    head_dim = triple // 3
    flat_weight = in_weight.reshape(in_weight.shape[0], head_count * triple)
    projected = jnp.dot(normed, flat_weight, preferred_element_type=jnp.float32).reshape(row_count, head_count, triple)
    queries = rms_gain(projected[..., :head_dim], query_gain)
    fresh_keys = rms_gain(projected[..., head_dim:2 * head_dim], key_gain)
    return jnp.concatenate([queries, fresh_keys, projected[..., 2 * head_dim:]], axis=-1).astype(jnp.bfloat16)

def reference(tokens, modulation, in_weight, query_gain, key_gain, out_weight, stale_cache, lengths):
    normed = (normalize_rows(tokens.astype(jnp.float32)) * (1.0 + modulation[1]) + modulation[0]).astype(jnp.bfloat16)
    fresh = project(normed, in_weight, query_gain, key_gain)
    queries = fresh[..., :HD]
    new_cache = fresh[..., HD:]
    positions = jnp.arange(SEQ, dtype=jnp.int32)
    patch_of = positions // PATCH_TOK
    live = positions % PATCH_TOK < lengths[patch_of]
    inv_root = 1.0 / math.sqrt(HD)

    def one_patch(patch_index):
        own_rows = (patch_of == patch_index)[:, None, None]
        sources = jnp.where(own_rows, new_cache, stale_cache)
        patch_queries = lax.dynamic_slice_in_dim(queries, (patch_index * PATCH_TOK).astype(jnp.int32), PATCH_TOK, 0)

        def one_head(operands):
            head_queries, head_sources = operands
            scores = jnp.dot(head_queries, head_sources[:, :HD].T, preferred_element_type=jnp.float32) * inv_root
            scores = jnp.where(live[None, :], scores, NEGATIVE)
            row_max = lax.optimization_barrier(jnp.max(scores, axis=1, keepdims=True))
            weights = jnp.where(live[None, :], jnp.exp(scores - row_max), 0.0)
            denominator = lax.optimization_barrier(jnp.sum(weights, axis=1, keepdims=True))
            summed = jnp.dot(weights.astype(jnp.bfloat16), head_sources[:, HD:], preferred_element_type=jnp.float32)
            return (summed / denominator).astype(jnp.bfloat16)
        return lax.map(one_head, (jnp.swapaxes(patch_queries, 0, 1), jnp.swapaxes(sources, 0, 1)))
    attended = lax.map(one_patch, jnp.arange(SEQ // PATCH_TOK, dtype=jnp.int32))
    attended = jnp.transpose(attended, (0, 2, 1, 3)).reshape(SEQ, H, HD)
    group_heads = H // HEAD_GROUPS
    attention = jnp.zeros((SEQ, D), jnp.float32)
    for group_index in range(HEAD_GROUPS):
        first_head = group_index * group_heads
        rows_part = attended[:, first_head:first_head + group_heads].reshape(SEQ, group_heads * HD)
        weight_part = out_weight[first_head:first_head + group_heads].reshape(group_heads * HD, D)
        partial_sum = jnp.dot(rows_part, weight_part, preferred_element_type=jnp.float32).astype(jnp.bfloat16)
        partial_sum = lax.optimization_barrier(partial_sum)
        attention = attention + partial_sum.astype(jnp.float32)
    update = (modulation[2] * attention).astype(jnp.bfloat16)
    return (update, new_cache)
```

```python
import functools
import math

import jax
import jax.numpy as jnp
from jax import lax
from jax.experimental import pallas as pl
from jax.experimental.pallas import tpu as pltpu
from jax.sharding import PartitionSpec as P

EPSILON = 1e-06
NEGATIVE = -1e30
key_block = 512


def normalize_rows(values):
    average = jnp.mean(values, axis=-1, keepdims=True)
    centred = values - average
    variance = jnp.mean(centred * centred, axis=-1, keepdims=True)
    return centred * lax.rsqrt(variance + EPSILON)


def rms_gain(values, gain):
    return values * lax.rsqrt(jnp.mean(values * values, axis=-1, keepdims=True) + EPSILON) * gain


def project(normed, in_weight, query_gain, key_gain):
    row_count = normed.shape[0]
    head_count = in_weight.shape[1]
    triple = in_weight.shape[2]
    head_dim = triple // 3
    flat_weight = in_weight.reshape(in_weight.shape[0], head_count * triple)
    projected = jnp.dot(normed, flat_weight, preferred_element_type=jnp.float32).reshape(
        row_count, head_count, triple
    )
    queries = rms_gain(projected[..., :head_dim], query_gain)
    fresh_keys = rms_gain(projected[..., head_dim : 2 * head_dim], key_gain)
    return jnp.concatenate([queries, fresh_keys, projected[..., 2 * head_dim :]], axis=-1).astype(
        jnp.bfloat16
    )


def lookup(lengths, patch_of):
    patch_ids = jnp.arange(lengths.shape[0], dtype=jnp.int32)
    return jnp.sum(jnp.where(patch_of[:, None] == patch_ids[None, :], lengths[None, :], 0), axis=1)


def attend(running, queries, key_rows, usable):
    head_dim = queries.shape[-1]
    row_max, denominator, weighted = running
    scores = jnp.einsum(
        "qhd,khd->qhk", queries, key_rows[..., :head_dim], preferred_element_type=jnp.float32
    )
    scores = scores * (1.0 / math.sqrt(head_dim))
    key_mask = usable[None, None, :]
    scores = jnp.where(key_mask, scores, NEGATIVE)
    new_max = jnp.maximum(row_max, jnp.max(scores, axis=-1))
    weights = jnp.where(key_mask, jnp.exp(scores - new_max[..., None]), 0.0)
    factor = jnp.exp(row_max - new_max)
    denominator = denominator * factor + jnp.sum(weights, axis=-1)
    weighted = weighted * factor[..., None] + jnp.einsum(
        "qhk,khd->qhd",
        weights.astype(jnp.bfloat16),
        key_rows[..., head_dim:],
        preferred_element_type=jnp.float32,
    )
    return (new_max, denominator, weighted)


def attend_blocks(running, queries, key_rows, usable):
    key_count = key_rows.shape[0]
    if key_count > key_block and key_count % key_block == 0:
        shaped = key_rows.reshape((key_count // key_block, key_block) + key_rows.shape[1:])
        usable_rows = usable.reshape(key_count // key_block, key_block)

        def step_block(current, operands):
            return (attend(current, queries, operands[0], operands[1]), None)

        running, _ = lax.scan(step_block, running, (shaped, usable_rows))
        return running
    return attend(running, queries, key_rows, usable)


def per_device(
    tokens, modulation, in_weight, query_gain, key_gain, out_weight, stale_cache, lengths
):
    heads_dev = in_weight.shape[1]
    head_dim = query_gain.shape[0]
    normed = (
        normalize_rows(tokens.astype(jnp.float32)) * (1.0 + modulation[1]) + modulation[0]
    ).astype(jnp.bfloat16)
    fresh = project(
        lax.all_gather(normed, ("head", "rep"), axis=0, tiled=True), in_weight, query_gain, key_gain
    )
    queries = fresh[..., :head_dim]
    own_rows = fresh[..., head_dim:]
    new_cache = lax.all_to_all(own_rows, ("head", "rep"), split_axis=0, concat_axis=1, tiled=True)
    patch_tok = fresh.shape[0]
    own_patch = lax.axis_index("patch")
    own_length = lookup(lengths, jnp.full((1,), own_patch, jnp.int32))[0]
    running = (
        jnp.full((patch_tok, heads_dev), NEGATIVE, jnp.float32),
        jnp.zeros((patch_tok, heads_dev), jnp.float32),
        jnp.zeros((patch_tok, heads_dev, head_dim), jnp.float32),
    )
    running = attend_blocks(
        running, queries, own_rows, jnp.arange(patch_tok, dtype=jnp.int32) < own_length
    )
    stale_heads = lax.all_to_all(
        stale_cache, ("head", "rep"), split_axis=1, concat_axis=0, tiled=True
    )
    shard_part = lax.all_gather(stale_heads, "patch", axis=0, tiled=True)
    key_index = jnp.arange(shard_part.shape[0], dtype=jnp.int32)
    patch_of = key_index // patch_tok
    position = key_index % patch_tok
    usable = (position < lookup(lengths, patch_of)) & (patch_of != own_patch)
    running = attend_blocks(running, queries, shard_part, usable)
    attended = (running[2] / running[1][..., None]).astype(jnp.bfloat16)
    flat_rows = attended.reshape(patch_tok, heads_dev * head_dim)
    flat_weight = out_weight.reshape(heads_dev * head_dim, out_weight.shape[2])
    attention = lax.psum_scatter(
        jnp.dot(flat_rows, flat_weight, preferred_element_type=jnp.float32).astype(jnp.bfloat16),
        ("head", "rep"),
        scatter_dimension=0,
        tiled=True,
    ).astype(jnp.float32)
    update = (modulation[2] * attention).astype(jnp.bfloat16)
    return (update, new_cache)


MESH = pl.DeviceIdType.MESH
K_CHUNKS = 4
OUT_CHUNKS = 4


def fused_kernel(
    tok, mod, qg, kg, lens, st, w_hbm, ow_hbm, upd, nc_out,
    w_raw, w_v, ow_v, st_t, normed_all, acc, stale_all, ncbuf, ncrecv, att, pbuf, dbuf, xs, xr,
    w_sem, ow_sem, st_send, st_recv, zs_r, zs_l, z_recv,
    na_s, nb_s, nr_s, n_recv, nc_s, nc_r, d_s, d_r, x_s, x_r,
    *, patches,
):
    p = lax.axis_index("patch")
    h = lax.axis_index("head")
    r = lax.axis_index("rep")
    heads = ow_hbm.shape[0]
    head_dim = ow_hbm.shape[1]
    rows, width = tok.shape
    triple = 3 * head_dim
    kc = width // K_CHUNKS
    oc = width // OUT_CHUNKS
    group = 4
    patch_tok = group * rows
    coords = [(h, r), (h, 1 - r), (1 - h, r), (1 - h, 1 - r)]
    slot = [a * 2 + b for a, b in coords]
    dev = [{"head": a, "rep": b} for a, b in coords]

    def remote(src, dst, ss, rs, to):
        return pltpu.make_async_remote_copy(
            src_ref=src, dst_ref=dst, send_sem=ss, recv_sem=rs, device_id=to, device_id_type=MESH
        )

    def w_copy(c):
        return pltpu.make_async_copy(
            w_hbm.at[pl.ds(c * kc, kc)], w_raw.at[pl.ds(c * kc, kc)], w_sem.at[c]
        )

    def w_turn(c):
        w_copy(c).wait()

        @pl.loop(0, kc // TURN)
        def _(i):
            at = pl.multiple_of(c * kc + i * TURN, TURN)
            w_v[:, pl.ds(at, TURN)] = jnp.transpose(w_raw[pl.ds(at, TURN)], (1, 0, 2))

    for c in range(K_CHUNKS):
        w_copy(c).start()
    ow_copy = pltpu.make_async_copy(ow_hbm, ow_v, ow_sem)
    ow_copy.start()

    has_right = p + 1 < patches
    has_left = p > 0
    barrier = pltpu.get_barrier_semaphore()
    for k in (1, 2, 3):
        pl.semaphore_signal(barrier, inc=1, device_id=dev[k], device_id_type=MESH)

    @pl.when(has_right)
    def _():
        pl.semaphore_signal(barrier, inc=1, device_id={"patch": p + 1}, device_id_type=MESH)

    @pl.when(has_left)
    def _():
        pl.semaphore_signal(barrier, inc=1, device_id={"patch": p - 1}, device_id_type=MESH)

    st_t[...] = jnp.transpose(st[...], (1, 0, 2))
    stale_all[p, slot[0]] = st_t[pl.ds(slot[0] * heads, heads)]
    values = tok[...].astype(jnp.float32)
    normed = (normalize_rows(values) * (1.0 + mod[1:2, :]) + mod[0:1, :]).astype(jnp.bfloat16)
    normed_all[slot[0]] = normed

    pl.semaphore_wait(barrier, 3 + has_right.astype(jnp.int32) + has_left.astype(jnp.int32))

    def stale_copy(k):
        return remote(
            st_t.at[pl.ds(slot[k] * heads, heads)], stale_all.at[p, slot[0]],
            st_send.at[k], st_recv.at[k], dev[k],
        )

    def stale_arrival(k):
        place = stale_all.at[p, slot[k]]
        remote(place, place, st_send.at[k], st_recv.at[k], dev[k]).wait_recv()

    def z_copy(q, k, right):
        place = stale_all.at[q, slot[k]]
        if right:
            return remote(place, place, zs_r.at[q, k], z_recv.at[q, k], {"patch": p + 1})
        return remote(place, place, zs_l.at[q, k], z_recv.at[q, k], {"patch": p - 1})

    def z_own(k):
        @pl.when(has_right)
        def _():
            z_copy(p, k, True).start()

        @pl.when(has_left)
        def _():
            z_copy(p, k, False).start()

    def z_relay(d, k):
        @pl.when(p - d >= 0)
        def _():
            z_copy(p - d, k, False).wait_recv()

            @pl.when(has_right)
            def _():
                z_copy(p - d, k, True).start()

        @pl.when(p + d < patches)
        def _():
            z_copy(p + d, k, True).wait_recv()

            @pl.when(has_left)
            def _():
                z_copy(p + d, k, False).start()

    def feature_copy(which, c):
        if which == 1:
            place = normed_all.at[slot[0], :, pl.ds(c * kc, kc)]
            return remote(place, place, na_s.at[c], n_recv.at[1, c], dev[1])
        if which == 2:
            place = normed_all.at[slot[0], :, pl.ds(c * kc, kc)]
            return remote(place, place, nb_s.at[c], n_recv.at[2, c], dev[2])
        place = normed_all.at[slot[2], :, pl.ds(c * kc, kc)]
        return remote(place, place, nr_s.at[c], n_recv.at[3, c], dev[1])

    def feature_arrival(k, c):
        place = normed_all.at[slot[k], :, pl.ds(c * kc, kc)]
        remote(place, place, na_s.at[c], n_recv.at[k, c], dev[1]).wait_recv()

    for k in (1, 2, 3):
        stale_copy(k).start()
    z_own(0)
    for c in range(K_CHUNKS):
        feature_copy(2, c).start()
        feature_copy(1, c).start()
    stale_arrival(1)
    z_own(1)
    w_turn(0)
    for k in (2, 3):
        stale_arrival(k)
        z_own(k)

    relays = [(d, k) for d in range(1, patches) for k in range(group)]
    early = 2 * K_CHUNKS
    for c in range(K_CHUNKS):
        feature_arrival(2, c)
        feature_copy(3, c).start()
        if c > 0:
            for d, k in relays[2 * (c - 1) : 2 * c]:
                z_relay(d, k)
        if c > 0:
            w_turn(c)
        feature_arrival(1, c)
        feature_arrival(3, c)
        part = normed_all[:, :, c * kc : (c + 1) * kc].reshape(patch_tok, kc)
        for j in range(heads):
            w_block = w_v[j, c * kc : (c + 1) * kc, :]
            product = jnp.dot(part, w_block, preferred_element_type=jnp.float32)
            if c == 0:
                acc[j] = product
            else:
                acc[j] += product

    for d, k in relays[early - 2 : early]:
        z_relay(d, k)

    q_gain = qg[...]
    k_gain = kg[...]
    queries = []
    for j in range(heads):
        queries.append(rms_gain(acc[j, :, :head_dim], q_gain).astype(jnp.bfloat16))
        keys = rms_gain(acc[j, :, head_dim : 2 * head_dim], k_gain).astype(jnp.bfloat16)
        ncbuf[:, j, :, :head_dim] = keys.reshape(group, rows, head_dim)
        ncbuf[:, j, :, head_dim:] = (
            acc[j, :, 2 * head_dim :].astype(jnp.bfloat16).reshape(group, rows, head_dim)
        )

    def cache_copy(k):
        return remote(
            ncbuf.at[slot[k]], ncrecv.at[slot[0]], nc_s.at[k], nc_r.at[k], dev[k]
        )

    for k in (2, 3, 1):
        cache_copy(k).start()
    scale = 1.0 / math.sqrt(head_dim)
    own_cols = lax.broadcasted_iota(jnp.int32, (1, patch_tok), 1)
    own_mask = own_cols < lens[p]
    other_mask = jnp.concatenate(
        [(own_cols < jnp.where(p == q, 0, lens[q])).astype(jnp.int32) for q in range(patches)],
        axis=1,
    ) > 0
    contract = (((1,), (1,)), ((), ()))
    own_scores = []
    for j in range(heads):
        own_k = ncbuf[:, j, :, :head_dim].reshape(patch_tok, head_dim)
        own_scores.append(
            lax.dot_general(queries[j], own_k, contract, preferred_element_type=jnp.float32)
        )
    for d, k in relays[early:]:
        z_relay(d, k)
    for j in range(heads):
        own_v = ncbuf[:, j, :, head_dim:].reshape(patch_tok, head_dim)
        far_k = stale_all[:, :, j, :, :head_dim].reshape(patches * patch_tok, head_dim)
        far_v = stale_all[:, :, j, :, head_dim:].reshape(patches * patch_tok, head_dim)
        s_far = lax.dot_general(queries[j], far_k, contract, preferred_element_type=jnp.float32)
        s_own = jnp.where(own_mask, own_scores[j] * scale, NEGATIVE)
        s_far = jnp.where(other_mask, s_far * scale, NEGATIVE)
        top = jnp.maximum(
            jnp.max(s_own, axis=1, keepdims=True), jnp.max(s_far, axis=1, keepdims=True)
        )
        w_own = jnp.where(own_mask, jnp.exp(s_own - top), 0.0)
        w_far = jnp.where(other_mask, jnp.exp(s_far - top), 0.0)
        denominator = jnp.sum(w_own, axis=1, keepdims=True) + jnp.sum(w_far, axis=1, keepdims=True)
        total = jnp.dot(
            w_own.astype(jnp.bfloat16), own_v, preferred_element_type=jnp.float32
        ) + jnp.dot(w_far.astype(jnp.bfloat16), far_v, preferred_element_type=jnp.float32)
        att[:, j * head_dim : (j + 1) * head_dim] = (total / denominator).astype(jnp.bfloat16)

    ow_copy.wait()

    def d_copy(c, i):
        return remote(
            pbuf.at[c, slot[1 + 2 * i]], dbuf.at[c, i], d_s.at[c, i], d_r.at[c, i], dev[1]
        )

    def x_copy(c):
        return remote(xs.at[c], xr.at[c], x_s.at[c], x_r.at[c], dev[2])

    def pair_sum(c):
        d_copy(c, 1).wait_recv()
        xs[c] = (
            pbuf[c, slot[2]].astype(jnp.float32) + dbuf[c, 1].astype(jnp.float32)
        ).astype(jnp.bfloat16)
        x_copy(c).start()

    rows_att = att[...]
    flat = heads * head_dim
    for c in range(OUT_CHUNKS):
        piece = jnp.dot(
            rows_att,
            ow_v[:, :, c * oc : (c + 1) * oc].reshape(flat, oc),
            preferred_element_type=jnp.float32,
        )
        pbuf[c] = piece.astype(jnp.bfloat16).reshape(group, rows, oc)
        d_copy(c, 1).start()
        d_copy(c, 0).start()
        if c > 0:
            pair_sum(c - 1)
    pair_sum(OUT_CHUNKS - 1)

    ncrecv[slot[0]] = ncbuf[slot[0]]
    for k in (1, 2, 3):
        place = ncrecv.at[slot[k]]
        remote(place, place, nc_s.at[k], nc_r.at[k], dev[k]).wait_recv()
    landed = ncrecv[...].reshape(group * heads, rows, 2 * head_dim)
    nc_out[...] = jnp.transpose(landed, (1, 0, 2))

    for c in range(OUT_CHUNKS):
        d_copy(c, 0).wait_recv()
        x_copy(c).wait_recv()
        total = (
            pbuf[c, slot[0]].astype(jnp.float32)
            + dbuf[c, 0].astype(jnp.float32)
            + xr[c].astype(jnp.float32)
        )
        upd[:, c * oc : (c + 1) * oc] = (mod[2:3, c * oc : (c + 1) * oc] * total).astype(
            jnp.bfloat16
        )

    for k in (1, 2, 3):
        stale_copy(k).wait_send()
        cache_copy(k).wait_send()
    for c in range(K_CHUNKS):
        for which in (1, 2, 3):
            feature_copy(which, c).wait_send()
    for c in range(OUT_CHUNKS):
        d_copy(c, 0).wait_send()
        d_copy(c, 1).wait_send()
        x_copy(c).wait_send()
    for q in range(patches):
        for k in range(group):

            @pl.when(has_right & (q <= p))
            def _():
                z_copy(q, k, True).wait_send()

            @pl.when(has_left & (q >= p))
            def _():
                z_copy(q, k, False).wait_send()


TURN = 32


def fused_device(
    patches, tokens, modulation, in_weight, query_gain, key_gain, out_weight, stale_cache, lengths
):
    rows, width = tokens.shape
    heads, head_dim = out_weight.shape[:2]
    group = 4
    all_heads = stale_cache.shape[1]
    patch_tok = rows * group
    bf, f32 = jnp.bfloat16, jnp.float32
    oc = width // OUT_CHUNKS
    vm = pl.BlockSpec(memory_space=pltpu.VMEM)
    anyspace = pl.BlockSpec(memory_space=pl.ANY)
    dma = pltpu.SemaphoreType.DMA
    upd, cache = pl.pallas_call(
        functools.partial(fused_kernel, patches=patches),
        out_shape=(
            jax.ShapeDtypeStruct((rows, width), bf),
            jax.ShapeDtypeStruct((rows, all_heads, 2 * head_dim), bf),
        ),
        in_specs=[vm, vm, vm, vm, pl.BlockSpec(memory_space=pltpu.SMEM), vm, anyspace, anyspace],
        out_specs=(vm, vm),
        scratch_shapes=[
            pltpu.VMEM(in_weight.shape, bf),
            pltpu.VMEM((heads, width, 3 * head_dim), bf),
            pltpu.VMEM(out_weight.shape, bf),
            pltpu.VMEM((all_heads, rows, 2 * head_dim), bf),
            pltpu.VMEM((group, rows, width), bf),
            pltpu.VMEM((heads, patch_tok, 3 * head_dim), f32),
            pltpu.VMEM((patches, group, heads, rows, 2 * head_dim), bf),
            pltpu.VMEM((group, heads, rows, 2 * head_dim), bf),
            pltpu.VMEM((group, heads, rows, 2 * head_dim), bf),
            pltpu.VMEM((patch_tok, heads * head_dim), bf),
            pltpu.VMEM((OUT_CHUNKS, group, rows, oc), bf),
            pltpu.VMEM((OUT_CHUNKS, 2, rows, oc), bf),
            pltpu.VMEM((OUT_CHUNKS, rows, oc), bf),
            pltpu.VMEM((OUT_CHUNKS, rows, oc), bf),
            dma((K_CHUNKS,)), dma, dma((4,)), dma((4,)),
            dma((patches, 4)), dma((patches, 4)), dma((patches, 4)),
            dma((K_CHUNKS,)), dma((K_CHUNKS,)), dma((K_CHUNKS,)), dma((4, K_CHUNKS)),
            dma((4,)), dma((4,)),
            dma((OUT_CHUNKS, 2)), dma((OUT_CHUNKS, 2)), dma((OUT_CHUNKS,)), dma((OUT_CHUNKS,)),
        ],
        compiler_params=pltpu.CompilerParams(
            collective_id=0, has_side_effects=True, vmem_limit_bytes=56 * 1024 * 1024
        ),
    )(
        tokens, modulation, query_gain.reshape(1, -1), key_gain.reshape(1, -1), lengths,
        stale_cache, in_weight, out_weight,
    )
    return upd, cache


def choose(
    patches, group_shape, tokens, modulation, in_weight, query_gain, key_gain, out_weight,
    stale_cache, lengths,
):
    rows, width = tokens.shape
    heads, head_dim = out_weight.shape[:2]
    kv_bytes = patches * 4 * heads * rows * 4 * head_dim
    weight_bytes = 2 * (in_weight.size + out_weight.size)
    fits = (
        group_shape == (2, 2)
        and rows % 16 == 0
        and head_dim % 128 == 0
        and width % (128 * K_CHUNKS) == 0
        and width % (128 * OUT_CHUNKS) == 0
        and rows * 4 * patches <= 1024
        and kv_bytes + weight_bytes <= 24 * 1024 * 1024
    )
    args = (
        tokens, modulation, in_weight, query_gain, key_gain, out_weight, stale_cache, lengths
    )
    return fused_device(patches, *args) if fits else per_device(*args)


def solution(mesh):
    return jax.shard_map(
        functools.partial(
            choose, mesh.shape["patch"], (mesh.shape["head"], mesh.shape["rep"])
        ),
        mesh=mesh,
        in_specs=(
            P(("clip", "patch", "head", "rep"), None),
            P(),
            P(None, ("head", "rep"), None),
            P(),
            P(),
            P(("head", "rep"), None, None),
            P(("clip", "patch", "head", "rep"), None, None),
            P("clip"),
        ),
        out_specs=(
            P(("clip", "patch", "head", "rep"), None),
            P(("clip", "patch", "head", "rep"), None, None),
        ),
        check_vma=False,
    )
```

```python
import functools
import math

import jax
import jax.numpy as jnp
from jax import lax
from jax.experimental import pallas as pl
from jax.experimental.pallas import tpu as pltpu
from jax.sharding import PartitionSpec as P

EPSILON = 1e-06
NEGATIVE = -1e30
key_block = 512


def normalize_rows(values):
    average = jnp.mean(values, axis=-1, keepdims=True)
    centred = values - average
    variance = jnp.mean(centred * centred, axis=-1, keepdims=True)
    return centred * lax.rsqrt(variance + EPSILON)


def rms_gain(values, gain):
    return values * lax.rsqrt(jnp.mean(values * values, axis=-1, keepdims=True) + EPSILON) * gain


def project(normed, in_weight, query_gain, key_gain):
    row_count = normed.shape[0]
    head_count = in_weight.shape[1]
    triple = in_weight.shape[2]
    head_dim = triple // 3
    flat_weight = in_weight.reshape(in_weight.shape[0], head_count * triple)
    projected = jnp.dot(normed, flat_weight, preferred_element_type=jnp.float32).reshape(
        row_count, head_count, triple
    )
    queries = rms_gain(projected[..., :head_dim], query_gain)
    fresh_keys = rms_gain(projected[..., head_dim : 2 * head_dim], key_gain)
    return jnp.concatenate([queries, fresh_keys, projected[..., 2 * head_dim :]], axis=-1).astype(
        jnp.bfloat16
    )


def lookup(lengths, patch_of):
    patch_ids = jnp.arange(lengths.shape[0], dtype=jnp.int32)
    return jnp.sum(jnp.where(patch_of[:, None] == patch_ids[None, :], lengths[None, :], 0), axis=1)


def attend(running, queries, key_rows, usable):
    head_dim = queries.shape[-1]
    row_max, denominator, weighted = running
    scores = jnp.einsum(
        "qhd,khd->qhk", queries, key_rows[..., :head_dim], preferred_element_type=jnp.float32
    )
    scores = scores * (1.0 / math.sqrt(head_dim))
    key_mask = usable[None, None, :]
    scores = jnp.where(key_mask, scores, NEGATIVE)
    new_max = jnp.maximum(row_max, jnp.max(scores, axis=-1))
    weights = jnp.where(key_mask, jnp.exp(scores - new_max[..., None]), 0.0)
    factor = jnp.exp(row_max - new_max)
    denominator = denominator * factor + jnp.sum(weights, axis=-1)
    weighted = weighted * factor[..., None] + jnp.einsum(
        "qhk,khd->qhd",
        weights.astype(jnp.bfloat16),
        key_rows[..., head_dim:],
        preferred_element_type=jnp.float32,
    )
    return (new_max, denominator, weighted)


def attend_blocks(running, queries, key_rows, usable):
    key_count = key_rows.shape[0]
    if key_count > key_block and key_count % key_block == 0:
        shaped = key_rows.reshape((key_count // key_block, key_block) + key_rows.shape[1:])
        usable_rows = usable.reshape(key_count // key_block, key_block)

        def step_block(current, operands):
            return (attend(current, queries, operands[0], operands[1]), None)

        running, _ = lax.scan(step_block, running, (shaped, usable_rows))
        return running
    return attend(running, queries, key_rows, usable)


def per_device(
    tokens, modulation, in_weight, query_gain, key_gain, out_weight, stale_cache, lengths
):
    heads_dev = in_weight.shape[1]
    head_dim = query_gain.shape[0]
    normed = (
        normalize_rows(tokens.astype(jnp.float32)) * (1.0 + modulation[1]) + modulation[0]
    ).astype(jnp.bfloat16)
    fresh = project(
        lax.all_gather(normed, ("head", "rep"), axis=0, tiled=True), in_weight, query_gain, key_gain
    )
    queries = fresh[..., :head_dim]
    own_rows = fresh[..., head_dim:]
    new_cache = lax.all_to_all(own_rows, ("head", "rep"), split_axis=0, concat_axis=1, tiled=True)
    patch_tok = fresh.shape[0]
    own_patch = lax.axis_index("patch")
    own_length = lookup(lengths, jnp.full((1,), own_patch, jnp.int32))[0]
    running = (
        jnp.full((patch_tok, heads_dev), NEGATIVE, jnp.float32),
        jnp.zeros((patch_tok, heads_dev), jnp.float32),
        jnp.zeros((patch_tok, heads_dev, head_dim), jnp.float32),
    )
    running = attend_blocks(
        running, queries, own_rows, jnp.arange(patch_tok, dtype=jnp.int32) < own_length
    )
    stale_heads = lax.all_to_all(
        stale_cache, ("head", "rep"), split_axis=1, concat_axis=0, tiled=True
    )
    shard_part = lax.all_gather(stale_heads, "patch", axis=0, tiled=True)
    key_index = jnp.arange(shard_part.shape[0], dtype=jnp.int32)
    patch_of = key_index // patch_tok
    position = key_index % patch_tok
    usable = (position < lookup(lengths, patch_of)) & (patch_of != own_patch)
    running = attend_blocks(running, queries, shard_part, usable)
    attended = (running[2] / running[1][..., None]).astype(jnp.bfloat16)
    flat_rows = attended.reshape(patch_tok, heads_dev * head_dim)
    flat_weight = out_weight.reshape(heads_dev * head_dim, out_weight.shape[2])
    attention = lax.psum_scatter(
        jnp.dot(flat_rows, flat_weight, preferred_element_type=jnp.float32).astype(jnp.bfloat16),
        ("head", "rep"),
        scatter_dimension=0,
        tiled=True,
    ).astype(jnp.float32)
    update = (modulation[2] * attention).astype(jnp.bfloat16)
    return (update, new_cache)


MESH = pl.DeviceIdType.MESH
K_CHUNKS = 4
OUT_CHUNKS = 4
TURN = 64


def nearest(p, patches, i):
    place = 0
    for own in range(patches):
        others = sorted((q for q in range(patches) if q != own), key=lambda q: (abs(q - own), q))
        place = place + (p == own).astype(jnp.int32) * others[i]
    return place


def fused_kernel(
    tok_hbm, mod_hbm, qg_hbm, kg_hbm, lens_hbm, st_hbm, w_hbm, ow_hbm, upd, nc_out,
    tok, mod, qg, kg, lens, st,
    w_raw, w_v, ow_v, st_t, normed_all, acc, stale_all, ncbuf, ncrecv,
    qbuf, top_v, den_v, out_v, att, pbuf, dbuf, xs, xr,
    in_sem, w_sem, ow_sem, st_send, st_recv, zs_r, zs_l, z_recv,
    na_s, nb_s, nr_s, n_recv, nc_s, nc_r, d_s, d_r, x_s, x_r,
    *, patches,
):
    p = lax.axis_index("patch")
    h = lax.axis_index("head")
    r = lax.axis_index("rep")
    heads = ow_hbm.shape[0]
    head_dim = ow_hbm.shape[1]
    rows, width = tok.shape
    triple = 3 * head_dim
    kc = width // K_CHUNKS
    oc = width // OUT_CHUNKS
    group = 4
    patch_tok = group * rows
    coords = [(h, r), (h, 1 - r), (1 - h, r), (1 - h, 1 - r)]
    slot = [a * 2 + b for a, b in coords]
    dev = [{"head": a, "rep": b} for a, b in coords]

    def remote(src, dst, ss, rs, to):
        return pltpu.make_async_remote_copy(
            src_ref=src, dst_ref=dst, send_sem=ss, recv_sem=rs, device_id=to, device_id_type=MESH
        )

    loads = [
        pltpu.make_async_copy(src, dst, in_sem.at[i])
        for i, (src, dst) in enumerate(
            [(st_hbm, st), (tok_hbm, tok), (mod_hbm, mod), (qg_hbm, qg), (kg_hbm, kg), (lens_hbm, lens)]
        )
    ]
    for load in loads:
        load.start()

    has_right = p + 1 < patches
    has_left = p > 0
    barrier = pltpu.get_barrier_semaphore()
    for k in (1, 2, 3):
        pl.semaphore_signal(barrier, inc=1, device_id=dev[k], device_id_type=MESH)

    @pl.when(has_right)
    def _():
        pl.semaphore_signal(barrier, inc=1, device_id={"patch": p + 1}, device_id_type=MESH)

    @pl.when(has_left)
    def _():
        pl.semaphore_signal(barrier, inc=1, device_id={"patch": p - 1}, device_id_type=MESH)

    def w_copy(c):
        return pltpu.make_async_copy(
            w_hbm.at[pl.ds(c * kc, kc)], w_raw.at[pl.ds(c * kc, kc)], w_sem.at[c]
        )

    def w_turn(c):
        w_copy(c).wait()

        @pl.loop(0, kc // TURN)
        def _(i):
            at = pl.multiple_of(c * kc + i * TURN, TURN)
            turned = jnp.transpose(w_raw[pl.ds(at, TURN)], (1, 0, 2))
            for j in range(heads):
                w_v[pl.ds(at, TURN), j * triple : (j + 1) * triple] = turned[j]

    for c in range(K_CHUNKS):
        w_copy(c).start()
    ow_copy = pltpu.make_async_copy(ow_hbm, ow_v, ow_sem)
    ow_copy.start()

    loads[0].wait()
    st_t[...] = jnp.transpose(st[...], (1, 0, 2))
    loads[1].wait()
    loads[2].wait()
    values = tok[...].astype(jnp.float32)
    normed = (normalize_rows(values) * (1.0 + mod[1:2, :]) + mod[0:1, :]).astype(jnp.bfloat16)
    normed_all[slot[0]] = normed

    pl.semaphore_wait(barrier, 3 + has_right.astype(jnp.int32) + has_left.astype(jnp.int32))

    def stale_part(k):
        return st_t.at[pl.ds(slot[k] * heads, heads)]

    def stale_copy(k):
        return remote(
            stale_part(k), stale_all.at[p, slot[0]], st_send.at[k], st_recv.at[k], dev[k]
        )

    def stale_arrival(k):
        place = stale_all.at[p, slot[k]]
        remote(place, place, st_send.at[k], st_recv.at[k], dev[k]).wait_recv()

    def z_copy(q, k, right, own=False):
        place = stale_all.at[q, slot[k]]
        src = stale_part(0) if own else place
        if right:
            return remote(src, place, zs_r.at[q, k], z_recv.at[q, k], {"patch": p + 1})
        return remote(src, place, zs_l.at[q, k], z_recv.at[q, k], {"patch": p - 1})

    def z_own(k):
        @pl.when(has_right)
        def _():
            z_copy(p, k, True, k == 0).start()

        @pl.when(has_left)
        def _():
            z_copy(p, k, False, k == 0).start()

    def z_relay(d, k):
        @pl.when(p - d >= 0)
        def _():
            z_copy(p - d, k, False).wait_recv()

            @pl.when(has_right)
            def _():
                z_copy(p - d, k, True).start()

        @pl.when(p + d < patches)
        def _():
            z_copy(p + d, k, True).wait_recv()

            @pl.when(has_left)
            def _():
                z_copy(p + d, k, False).start()

    def feature_copy(which, c):
        if which == 1:
            place = normed_all.at[slot[0], :, pl.ds(c * kc, kc)]
            return remote(place, place, na_s.at[c], n_recv.at[1, c], dev[1])
        if which == 2:
            place = normed_all.at[slot[0], :, pl.ds(c * kc, kc)]
            return remote(place, place, nb_s.at[c], n_recv.at[2, c], dev[2])
        place = normed_all.at[slot[2], :, pl.ds(c * kc, kc)]
        return remote(place, place, nr_s.at[c], n_recv.at[3, c], dev[1])

    def feature_arrival(k, c):
        place = normed_all.at[slot[k], :, pl.ds(c * kc, kc)]
        remote(place, place, na_s.at[c], n_recv.at[k, c], dev[1]).wait_recv()

    relays = [(d, k) for d in range(1, patches) for k in range(group)]
    done = [0]

    def relay_to(count):
        for d, k in relays[done[0] : count]:
            z_relay(d, k)
        done[0] = max(done[0], count)

    z_own(0)
    for k in (1, 2, 3):
        stale_copy(k).start()
    for c in range(K_CHUNKS):
        feature_copy(2, c).start()
        feature_copy(1, c).start()
    stale_arrival(1)
    z_own(1)
    w_turn(0)
    stale_arrival(2)
    z_own(2)
    w_turn(1)
    stale_arrival(3)
    z_own(3)
    relay_to(1)
    for c in range(2, K_CHUNKS):
        w_turn(c)

    relay_to(2)
    feature_arrival(2, 0)
    feature_copy(3, 0).start()
    for c in range(K_CHUNKS):
        if c + 1 < K_CHUNKS:
            feature_arrival(2, c + 1)
            feature_copy(3, c + 1).start()
        feature_arrival(1, c)
        feature_arrival(3, c)
        part = normed_all[:, :, c * kc : (c + 1) * kc].reshape(patch_tok, kc)
        product = jnp.dot(
            part, w_v[c * kc : (c + 1) * kc, :], preferred_element_type=jnp.float32
        )
        if c == 0:
            acc[...] = product
        else:
            acc[...] += product
        relay_to(min(group, 3 + c))

    for load in loads[3:]:
        load.wait()
    q_gain = qg[...]
    k_gain = kg[...]
    for j in range(heads):
        base = j * triple
        keys = rms_gain(acc[:, base + head_dim : base + 2 * head_dim], k_gain).astype(jnp.bfloat16)
        ncbuf[:, j, :, :head_dim] = keys.reshape(group, rows, head_dim)
        ncbuf[:, j, :, head_dim:] = (
            acc[:, base + 2 * head_dim : base + triple]
            .astype(jnp.bfloat16)
            .reshape(group, rows, head_dim)
        )
        qbuf[j] = rms_gain(acc[:, base : base + head_dim], q_gain).astype(jnp.bfloat16)

    def cache_copy(k):
        return remote(
            ncbuf.at[slot[k]], ncrecv.at[slot[0]], nc_s.at[k], nc_r.at[k], dev[k]
        )

    for k in (2, 3, 1):
        cache_copy(k).start()
    relay_to(group + 1)
    scale = 1.0 / math.sqrt(head_dim)
    columns = lax.broadcasted_iota(jnp.int32, (1, patch_tok), 1)
    contract = (((1,), (1,)), ((), ()))

    def attend_part(sources, first, last):
        masks = [columns < live for _, live in sources]
        scores = [
            [
                lax.dot_general(
                    qbuf[j],
                    source[:, j, :, :head_dim].reshape(patch_tok, head_dim),
                    contract,
                    preferred_element_type=jnp.float32,
                )
                for source, _ in sources
            ]
            for j in range(heads)
        ]
        scores = [
            [jnp.where(mask, part * scale, NEGATIVE) for part, mask in zip(scores[j], masks)]
            for j in range(heads)
        ]
        tops = [
            functools.reduce(
                jnp.maximum, [jnp.max(part, axis=1, keepdims=True) for part in scores[j]]
            )
            for j in range(heads)
        ]
        if not first:
            before = [top_v[j] for j in range(heads)]
            tops = [jnp.maximum(before[j], tops[j]) for j in range(heads)]
            factor = [jnp.exp(before[j] - tops[j]) for j in range(heads)]
        weights = [
            [
                jnp.where(mask, jnp.exp(part - tops[j]), 0.0)
                for part, mask in zip(scores[j], masks)
            ]
            for j in range(heads)
        ]
        mixed = [
            sum(
                jnp.dot(
                    part.astype(jnp.bfloat16),
                    source[:, j, :, head_dim:].reshape(patch_tok, head_dim),
                    preferred_element_type=jnp.float32,
                )
                for part, (source, _) in zip(weights[j], sources)
            )
            for j in range(heads)
        ]
        total = [
            sum(jnp.sum(part, axis=1, keepdims=True) for part in weights[j]) for j in range(heads)
        ]
        if not first:
            total = [total[j] + den_v[j] * factor[j] for j in range(heads)]
            mixed = [mixed[j] + out_v[j] * factor[j] for j in range(heads)]
        for j in range(heads):
            if last:
                att[:, j * head_dim : (j + 1) * head_dim] = (mixed[j] / total[j]).astype(
                    jnp.bfloat16
                )
            else:
                top_v[j] = tops[j]
                den_v[j] = total[j]
                out_v[j] = mixed[j]

    def other(i):
        q = nearest(p, patches, i)
        return stale_all.at[q], lens[q]

    attend_part([(ncbuf, lens[p])], True, False)
    relay_to(group * (patches - 2))
    if patches > 2:
        attend_part([other(i) for i in range(patches - 2)], False, False)
    relay_to(group * (patches - 1))
    attend_part([other(patches - 2)], False, True)

    ow_copy.wait()

    def d_copy(c, i):
        return remote(
            pbuf.at[c, slot[1 + 2 * i]], dbuf.at[c, i], d_s.at[c, i], d_r.at[c, i], dev[1]
        )

    def x_copy(c):
        return remote(xs.at[c], xr.at[c], x_s.at[c], x_r.at[c], dev[2])

    def pair_sum(c):
        d_copy(c, 1).wait_recv()
        xs[c] = (
            pbuf[c, slot[2]].astype(jnp.float32) + dbuf[c, 1].astype(jnp.float32)
        ).astype(jnp.bfloat16)
        x_copy(c).start()

    rows_att = att[...]
    flat = heads * head_dim
    for c in range(OUT_CHUNKS):
        piece = jnp.dot(
            rows_att,
            ow_v[:, :, c * oc : (c + 1) * oc].reshape(flat, oc),
            preferred_element_type=jnp.float32,
        )
        pbuf[c] = piece.astype(jnp.bfloat16).reshape(group, rows, oc)
        d_copy(c, 1).start()
        d_copy(c, 0).start()
        if c > 0:
            pair_sum(c - 1)
    pair_sum(OUT_CHUNKS - 1)

    ncrecv[slot[0]] = ncbuf[slot[0]]
    for k in (1, 2, 3):
        place = ncrecv.at[slot[k]]
        remote(place, place, nc_s.at[k], nc_r.at[k], dev[k]).wait_recv()
    landed = ncrecv[...].reshape(group * heads, rows, 2 * head_dim)
    nc_out[...] = jnp.transpose(landed, (1, 0, 2))

    for k in (1, 2, 3):
        stale_copy(k).wait_send()
        cache_copy(k).wait_send()
    for c in range(K_CHUNKS):
        for which in (1, 2, 3):
            feature_copy(which, c).wait_send()
    for q in range(patches):
        for k in range(group):

            @pl.when(has_right & (q <= p))
            def _():
                z_copy(q, k, True).wait_send()

            @pl.when(has_left & (q >= p))
            def _():
                z_copy(q, k, False).wait_send()

    for c in range(OUT_CHUNKS):
        d_copy(c, 0).wait_recv()
        x_copy(c).wait_recv()
        total = (
            pbuf[c, slot[0]].astype(jnp.float32)
            + dbuf[c, 0].astype(jnp.float32)
            + xr[c].astype(jnp.float32)
        )
        upd[:, c * oc : (c + 1) * oc] = (mod[2:3, c * oc : (c + 1) * oc] * total).astype(
            jnp.bfloat16
        )
    for c in range(OUT_CHUNKS):
        d_copy(c, 0).wait_send()
        d_copy(c, 1).wait_send()
        x_copy(c).wait_send()


def fused_device(
    patches, tokens, modulation, in_weight, query_gain, key_gain, out_weight, stale_cache, lengths
):
    rows, width = tokens.shape
    heads, head_dim = out_weight.shape[:2]
    group = 4
    all_heads = stale_cache.shape[1]
    patch_tok = rows * group
    bf, f32 = jnp.bfloat16, jnp.float32
    oc = width // OUT_CHUNKS
    vm = pl.BlockSpec(memory_space=pltpu.VMEM)
    dma = pltpu.SemaphoreType.DMA
    return pl.pallas_call(
        functools.partial(fused_kernel, patches=patches),
        out_shape=(
            jax.ShapeDtypeStruct((rows, width), bf),
            jax.ShapeDtypeStruct((rows, all_heads, 2 * head_dim), bf),
        ),
        in_specs=[pl.BlockSpec(memory_space=pltpu.HBM)] * 8,
        out_specs=(vm, vm),
        scratch_shapes=[
            pltpu.VMEM(tokens.shape, bf),
            pltpu.VMEM(modulation.shape, f32),
            pltpu.VMEM((1, head_dim), f32),
            pltpu.VMEM((1, head_dim), f32),
            pltpu.SMEM(lengths.shape, jnp.int32),
            pltpu.VMEM(stale_cache.shape, bf),
            pltpu.VMEM(in_weight.shape, bf),
            pltpu.VMEM((width, heads * 3 * head_dim), bf),
            pltpu.VMEM(out_weight.shape, bf),
            pltpu.VMEM((all_heads, rows, 2 * head_dim), bf),
            pltpu.VMEM((group, rows, width), bf),
            pltpu.VMEM((patch_tok, heads * 3 * head_dim), f32),
            pltpu.VMEM((patches, group, heads, rows, 2 * head_dim), bf),
            pltpu.VMEM((group, heads, rows, 2 * head_dim), bf),
            pltpu.VMEM((group, heads, rows, 2 * head_dim), bf),
            pltpu.VMEM((heads, patch_tok, head_dim), bf),
            pltpu.VMEM((heads, patch_tok, 1), f32),
            pltpu.VMEM((heads, patch_tok, 1), f32),
            pltpu.VMEM((heads, patch_tok, head_dim), f32),
            pltpu.VMEM((patch_tok, heads * head_dim), bf),
            pltpu.VMEM((OUT_CHUNKS, group, rows, oc), bf),
            pltpu.VMEM((OUT_CHUNKS, 2, rows, oc), bf),
            pltpu.VMEM((OUT_CHUNKS, rows, oc), bf),
            pltpu.VMEM((OUT_CHUNKS, rows, oc), bf),
            dma((6,)), dma((K_CHUNKS,)), dma, dma((4,)), dma((4,)),
            dma((patches, 4)), dma((patches, 4)), dma((patches, 4)),
            dma((K_CHUNKS,)), dma((K_CHUNKS,)), dma((K_CHUNKS,)), dma((4, K_CHUNKS)),
            dma((4,)), dma((4,)),
            dma((OUT_CHUNKS, 2)), dma((OUT_CHUNKS, 2)), dma((OUT_CHUNKS,)), dma((OUT_CHUNKS,)),
        ],
        compiler_params=pltpu.CompilerParams(
            collective_id=0, has_side_effects=True, vmem_limit_bytes=48 * 1024 * 1024
        ),
    )(
        *[
            pltpu.with_memory_space_constraint(operand, pltpu.HBM)
            for operand in (
                tokens, modulation, query_gain.reshape(1, -1), key_gain.reshape(1, -1), lengths,
                stale_cache, in_weight, out_weight,
            )
        ]
    )


def choose(
    patches, group_shape, tokens, modulation, in_weight, query_gain, key_gain, out_weight,
    stale_cache, lengths,
):
    rows, width = tokens.shape
    heads, head_dim = out_weight.shape[:2]
    kv_bytes = patches * 4 * heads * rows * 4 * head_dim
    weight_bytes = 2 * (in_weight.size + out_weight.size)
    fits = (
        group_shape == (2, 2)
        and rows % 16 == 0
        and head_dim % 128 == 0
        and width % (128 * K_CHUNKS) == 0
        and width % (128 * OUT_CHUNKS) == 0
        and width % (TURN * K_CHUNKS) == 0
        and patches > 1
        and rows * 4 * patches <= 1024
        and kv_bytes + weight_bytes <= 24 * 1024 * 1024
    )
    args = (
        tokens, modulation, in_weight, query_gain, key_gain, out_weight, stale_cache, lengths
    )
    return fused_device(patches, *args) if fits else per_device(*args)


def solution(mesh):
    return jax.shard_map(
        functools.partial(
            choose, mesh.shape["patch"], (mesh.shape["head"], mesh.shape["rep"])
        ),
        mesh=mesh,
        in_specs=(
            P(("clip", "patch", "head", "rep"), None),
            P(),
            P(None, ("head", "rep"), None),
            P(),
            P(),
            P(("head", "rep"), None, None),
            P(("clip", "patch", "head", "rep"), None, None),
            P("clip"),
        ),
        out_specs=(
            P(("clip", "patch", "head", "rep"), None),
            P(("clip", "patch", "head", "rep"), None, None),
        ),
        check_vma=False,
    )
```

```python
import functools
import math

import jax
import jax.numpy as jnp
from jax import lax
from jax.experimental import pallas as pl
from jax.experimental.pallas import tpu as pltpu
from jax.sharding import PartitionSpec as P

EPSILON = 1e-06
NEGATIVE = -1e30
key_block = 512


def normalize_rows(values):
    average = jnp.mean(values, axis=-1, keepdims=True)
    centred = values - average
    variance = jnp.mean(centred * centred, axis=-1, keepdims=True)
    return centred * lax.rsqrt(variance + EPSILON)


def rms_gain(values, gain):
    return values * lax.rsqrt(jnp.mean(values * values, axis=-1, keepdims=True) + EPSILON) * gain


def project(normed, in_weight, query_gain, key_gain):
    row_count = normed.shape[0]
    head_count = in_weight.shape[1]
    triple = in_weight.shape[2]
    head_dim = triple // 3
    flat_weight = in_weight.reshape(in_weight.shape[0], head_count * triple)
    projected = jnp.dot(normed, flat_weight, preferred_element_type=jnp.float32).reshape(
        row_count, head_count, triple
    )
    queries = rms_gain(projected[..., :head_dim], query_gain)
    fresh_keys = rms_gain(projected[..., head_dim : 2 * head_dim], key_gain)
    return jnp.concatenate([queries, fresh_keys, projected[..., 2 * head_dim :]], axis=-1).astype(
        jnp.bfloat16
    )


def lookup(lengths, patch_of):
    patch_ids = jnp.arange(lengths.shape[0], dtype=jnp.int32)
    return jnp.sum(jnp.where(patch_of[:, None] == patch_ids[None, :], lengths[None, :], 0), axis=1)


def attend(running, queries, key_rows, usable):
    head_dim = queries.shape[-1]
    row_max, denominator, weighted = running
    scores = jnp.einsum(
        "qhd,khd->qhk", queries, key_rows[..., :head_dim], preferred_element_type=jnp.float32
    )
    scores = scores * (1.0 / math.sqrt(head_dim))
    key_mask = usable[None, None, :]
    scores = jnp.where(key_mask, scores, NEGATIVE)
    new_max = jnp.maximum(row_max, jnp.max(scores, axis=-1))
    weights = jnp.where(key_mask, jnp.exp(scores - new_max[..., None]), 0.0)
    factor = jnp.exp(row_max - new_max)
    denominator = denominator * factor + jnp.sum(weights, axis=-1)
    weighted = weighted * factor[..., None] + jnp.einsum(
        "qhk,khd->qhd",
        weights.astype(jnp.bfloat16),
        key_rows[..., head_dim:],
        preferred_element_type=jnp.float32,
    )
    return (new_max, denominator, weighted)


def attend_blocks(running, queries, key_rows, usable):
    key_count = key_rows.shape[0]
    if key_count > key_block and key_count % key_block == 0:
        shaped = key_rows.reshape((key_count // key_block, key_block) + key_rows.shape[1:])
        usable_rows = usable.reshape(key_count // key_block, key_block)

        def step_block(current, operands):
            return (attend(current, queries, operands[0], operands[1]), None)

        running, _ = lax.scan(step_block, running, (shaped, usable_rows))
        return running
    return attend(running, queries, key_rows, usable)


def per_device(
    tokens, modulation, in_weight, query_gain, key_gain, out_weight, stale_cache, lengths
):
    heads_dev = in_weight.shape[1]
    head_dim = query_gain.shape[0]
    normed = (
        normalize_rows(tokens.astype(jnp.float32)) * (1.0 + modulation[1]) + modulation[0]
    ).astype(jnp.bfloat16)
    fresh = project(
        lax.all_gather(normed, ("head", "rep"), axis=0, tiled=True), in_weight, query_gain, key_gain
    )
    queries = fresh[..., :head_dim]
    own_rows = fresh[..., head_dim:]
    new_cache = lax.all_to_all(own_rows, ("head", "rep"), split_axis=0, concat_axis=1, tiled=True)
    patch_tok = fresh.shape[0]
    own_patch = lax.axis_index("patch")
    own_length = lookup(lengths, jnp.full((1,), own_patch, jnp.int32))[0]
    running = (
        jnp.full((patch_tok, heads_dev), NEGATIVE, jnp.float32),
        jnp.zeros((patch_tok, heads_dev), jnp.float32),
        jnp.zeros((patch_tok, heads_dev, head_dim), jnp.float32),
    )
    running = attend_blocks(
        running, queries, own_rows, jnp.arange(patch_tok, dtype=jnp.int32) < own_length
    )
    stale_heads = lax.all_to_all(
        stale_cache, ("head", "rep"), split_axis=1, concat_axis=0, tiled=True
    )
    shard_part = lax.all_gather(stale_heads, "patch", axis=0, tiled=True)
    key_index = jnp.arange(shard_part.shape[0], dtype=jnp.int32)
    patch_of = key_index // patch_tok
    position = key_index % patch_tok
    usable = (position < lookup(lengths, patch_of)) & (patch_of != own_patch)
    running = attend_blocks(running, queries, shard_part, usable)
    attended = (running[2] / running[1][..., None]).astype(jnp.bfloat16)
    flat_rows = attended.reshape(patch_tok, heads_dev * head_dim)
    flat_weight = out_weight.reshape(heads_dev * head_dim, out_weight.shape[2])
    attention = lax.psum_scatter(
        jnp.dot(flat_rows, flat_weight, preferred_element_type=jnp.float32).astype(jnp.bfloat16),
        ("head", "rep"),
        scatter_dimension=0,
        tiled=True,
    ).astype(jnp.float32)
    update = (modulation[2] * attention).astype(jnp.bfloat16)
    return (update, new_cache)


MESH = pl.DeviceIdType.MESH
K_CHUNKS = 4
OUT_SPLIT = (3, 4, 5, 6, 6)
TURN = 64


def nearest(p, patches, i):
    place = 0
    for own in range(patches):
        others = sorted((q for q in range(patches) if q != own), key=lambda q: (abs(q - own), q))
        place = place + (p == own).astype(jnp.int32) * others[i]
    return place


def fused_kernel(
    tok_hbm, mod_hbm, qg_hbm, kg_hbm, lens_hbm, st_hbm, w_hbm, ow_hbm, upd, nc_out,
    tok, mod, qg, kg, lens, st,
    w_raw, w_v, ow_v, st_t, normed_all, acc, stale_all, ncbuf, ncrecv,
    qbuf, top_v, den_v, out_v, att, pbuf, dbuf, raw, xs, xr,
    in_sem, w_sem, ow_sem, st_send, st_recv, zs_r, zs_l, z_recv,
    na_s, nb_s, nr_s, na_r, nb_r, nr_r, nc_s, nc_r,
    d_s, d_r, e_s, e_r, raw_s, raw_r, x_s, x_r,
    *, patches,
):
    p = lax.axis_index("patch")
    h = lax.axis_index("head")
    r = lax.axis_index("rep")
    heads = ow_hbm.shape[0]
    head_dim = ow_hbm.shape[1]
    rows, width = tok.shape
    triple = 3 * head_dim
    kc = width // K_CHUNKS
    group = 4
    patch_tok = group * rows
    coords = [(h, r), (h, 1 - r), (1 - h, r), (1 - h, 1 - r)]
    slot = [a * 2 + b for a, b in coords]
    dev = [{"head": a, "rep": b} for a, b in coords]

    def remote(src, dst, ss, rs, to):
        return pltpu.make_async_remote_copy(
            src_ref=src, dst_ref=dst, send_sem=ss, recv_sem=rs, device_id=to, device_id_type=MESH
        )

    loads = [
        pltpu.make_async_copy(src, dst, in_sem.at[i])
        for i, (src, dst) in enumerate(
            [(st_hbm, st), (tok_hbm, tok), (mod_hbm, mod), (qg_hbm, qg), (kg_hbm, kg), (lens_hbm, lens)]
        )
    ]
    for load in loads:
        load.start()

    has_right = p + 1 < patches
    has_left = p > 0
    barrier = pltpu.get_barrier_semaphore()
    for k in (1, 2, 3):
        pl.semaphore_signal(barrier, inc=1, device_id=dev[k], device_id_type=MESH)

    @pl.when(has_right)
    def _():
        pl.semaphore_signal(barrier, inc=1, device_id={"patch": p + 1}, device_id_type=MESH)

    @pl.when(has_left)
    def _():
        pl.semaphore_signal(barrier, inc=1, device_id={"patch": p - 1}, device_id_type=MESH)

    def w_copy(c):
        return pltpu.make_async_copy(
            w_hbm.at[pl.ds(c * kc, kc)], w_raw.at[pl.ds(c * kc, kc)], w_sem.at[c]
        )

    def w_turn(c):
        w_copy(c).wait()

        @pl.loop(0, kc // TURN)
        def _(i):
            at = pl.multiple_of(c * kc + i * TURN, TURN)
            turned = jnp.transpose(w_raw[pl.ds(at, TURN)], (1, 0, 2))
            for j in range(heads):
                w_v[pl.ds(at, TURN), j * triple : (j + 1) * triple] = turned[j]

    for c in range(K_CHUNKS):
        w_copy(c).start()
    ow_copy = pltpu.make_async_copy(ow_hbm, ow_v, ow_sem)
    ow_copy.start()

    loads[0].wait()
    st_t[...] = jnp.transpose(st[...], (1, 0, 2))

    pl.semaphore_wait(barrier, 3 + has_right.astype(jnp.int32) + has_left.astype(jnp.int32))

    def stale_part(k):
        return st_t.at[pl.ds(slot[k] * heads, heads)]

    def stale_copy(k):
        return remote(
            stale_part(k), stale_all.at[p, slot[0]], st_send, st_recv.at[k - 1], dev[k]
        )

    def stale_arrival(k):
        place = stale_all.at[p, slot[k]]
        remote(place, place, st_send, st_recv.at[k - 1], dev[k]).wait_recv()

    def z_copy(q, k, right, own=False):
        place = stale_all.at[q, slot[k]]
        src = stale_part(0) if own else place
        if right:
            return remote(src, place, zs_r.at[q], z_recv.at[q, k], {"patch": p + 1})
        return remote(src, place, zs_l.at[q], z_recv.at[q, k], {"patch": p - 1})

    def z_own(k):
        @pl.when(has_right)
        def _():
            z_copy(p, k, True, k == 0).start()

        @pl.when(has_left)
        def _():
            z_copy(p, k, False, k == 0).start()

    def z_relay(d, k):
        @pl.when(p - d >= 0)
        def _():
            z_copy(p - d, k, False).wait_recv()

            @pl.when(has_right)
            def _():
                z_copy(p - d, k, True).start()

        @pl.when(p + d < patches)
        def _():
            z_copy(p + d, k, True).wait_recv()

            @pl.when(has_left)
            def _():
                z_copy(p + d, k, False).start()

    def chunk(k, c):
        return normed_all.at[slot[k], :, pl.ds(c * kc, kc)]

    def feature_across(c):
        return remote(chunk(0, c), chunk(0, c), nb_s, nb_r.at[c], dev[2])

    def feature_beside():
        place = normed_all.at[slot[0]]
        return remote(place, place, na_s, na_r, dev[1])

    def feature_relay(c):
        return remote(chunk(2, c), chunk(2, c), nr_s, nr_r.at[c], dev[1])

    def feature_pass(c):
        remote(chunk(2, c), chunk(2, c), nb_s, nb_r.at[c], dev[2]).wait_recv()
        feature_relay(c).start()

    relays = [(d, k) for d in range(1, patches) for k in range(group)]
    done = [0]

    def relay_to(count):
        for d, k in relays[done[0] : count]:
            z_relay(d, k)
        done[0] = max(done[0], count)

    z_own(0)
    for k in (2, 3, 1):
        stale_copy(k).start()
    loads[1].wait()
    loads[2].wait()
    values = tok[...].astype(jnp.float32)
    normed = (normalize_rows(values) * (1.0 + mod[1:2, :]) + mod[0:1, :]).astype(jnp.bfloat16)
    normed_all[slot[0]] = normed
    for c in range(K_CHUNKS):
        feature_across(c).start()
    feature_beside().start()
    stale_arrival(1)
    z_own(1)
    w_turn(0)
    w_turn(1)
    stale_arrival(2)
    z_own(2)
    w_turn(2)
    stale_arrival(3)
    z_own(3)
    relay_to(1)
    for c in range(3, K_CHUNKS):
        w_turn(c)
    relay_to(2)
    feature_pass(0)
    beside = normed_all.at[slot[1]]
    remote(beside, beside, na_s, na_r, dev[1]).wait_recv()
    for c in range(K_CHUNKS):
        if c + 1 < K_CHUNKS:
            feature_pass(c + 1)
        remote(chunk(3, c), chunk(3, c), nr_s, nr_r.at[c], dev[1]).wait_recv()
        part = normed_all[:, :, c * kc : (c + 1) * kc].reshape(patch_tok, kc)
        product = jnp.dot(
            part, w_v[c * kc : (c + 1) * kc, :], preferred_element_type=jnp.float32
        )
        if c == 0:
            acc[...] = product
        else:
            acc[...] += product
        relay_to(min(group, 3 + c))

    for load in loads[3:]:
        load.wait()
    q_gain = qg[...]
    k_gain = kg[...]
    for j in range(heads):
        base = j * triple
        keys = rms_gain(acc[:, base + head_dim : base + 2 * head_dim], k_gain).astype(jnp.bfloat16)
        ncbuf[:, j, :, :head_dim] = keys.reshape(group, rows, head_dim)
        ncbuf[:, j, :, head_dim:] = (
            acc[:, base + 2 * head_dim : base + triple]
            .astype(jnp.bfloat16)
            .reshape(group, rows, head_dim)
        )
        qbuf[j] = rms_gain(acc[:, base : base + head_dim], q_gain).astype(jnp.bfloat16)

    def cache_copy(k):
        return remote(
            ncbuf.at[slot[k]], ncrecv.at[slot[0]], nc_s, nc_r, dev[k]
        )

    for k in (2, 3, 1):
        cache_copy(k).start()
    relay_to(group + 1)
    scale = 1.0 / math.sqrt(head_dim)
    columns = lax.broadcasted_iota(jnp.int32, (1, patch_tok), 1)
    contract = (((1,), (1,)), ((), ()))

    def attend_part(sources, first, last):
        masks = [columns < live for _, live in sources]
        scores = [
            [
                lax.dot_general(
                    qbuf[j],
                    source[:, j, :, :head_dim].reshape(patch_tok, head_dim),
                    contract,
                    preferred_element_type=jnp.float32,
                )
                for source, _ in sources
            ]
            for j in range(heads)
        ]
        scores = [
            [jnp.where(mask, part * scale, NEGATIVE) for part, mask in zip(scores[j], masks)]
            for j in range(heads)
        ]
        tops = [
            functools.reduce(
                jnp.maximum, [jnp.max(part, axis=1, keepdims=True) for part in scores[j]]
            )
            for j in range(heads)
        ]
        if not first:
            before = [top_v[j] for j in range(heads)]
            tops = [jnp.maximum(before[j], tops[j]) for j in range(heads)]
            factor = [jnp.exp(before[j] - tops[j]) for j in range(heads)]
        weights = [
            [
                jnp.where(mask, jnp.exp(part - tops[j]), 0.0)
                for part, mask in zip(scores[j], masks)
            ]
            for j in range(heads)
        ]
        mixed = [
            sum(
                jnp.dot(
                    part.astype(jnp.bfloat16),
                    source[:, j, :, head_dim:].reshape(patch_tok, head_dim),
                    preferred_element_type=jnp.float32,
                )
                for part, (source, _) in zip(weights[j], sources)
            )
            for j in range(heads)
        ]
        total = [
            sum(jnp.sum(part, axis=1, keepdims=True) for part in weights[j]) for j in range(heads)
        ]
        if not first:
            total = [total[j] + den_v[j] * factor[j] for j in range(heads)]
            mixed = [mixed[j] + out_v[j] * factor[j] for j in range(heads)]
        for j in range(heads):
            if last:
                att[:, j * head_dim : (j + 1) * head_dim] = (mixed[j] / total[j]).astype(
                    jnp.bfloat16
                )
            else:
                top_v[j] = tops[j]
                den_v[j] = total[j]
                out_v[j] = mixed[j]

    def other(i):
        q = nearest(p, patches, i)
        return stale_all.at[q], lens[q]

    attend_part([(ncbuf, lens[p])], True, False)
    relay_to(group * (patches - 2))
    if patches > 2:
        attend_part([other(i) for i in range(patches - 2)], False, False)
    relay_to(group * (patches - 1))
    attend_part([other(patches - 2)], False, True)

    ow_copy.wait()

    cuts = []
    for units in OUT_SPLIT:
        begin = cuts[-1].stop if cuts else 0
        cuts.append(slice(begin, begin + units * (width // sum(OUT_SPLIT))))
    ranges = [pl.ds(cut.start, cut.stop - cut.start) for cut in cuts]

    def near_copy(c):
        cols = ranges[c]
        return remote(pbuf.at[slot[1], :, cols], dbuf.at[0, :, cols], d_s, d_r, dev[1])

    def pair_copy(c):
        cols = ranges[c]
        return remote(pbuf.at[slot[3], :, cols], dbuf.at[1, :, cols], e_s, e_r.at[c - 1], dev[1])

    def raw_copy(k):
        cols = ranges[0]
        return remote(pbuf.at[slot[k], :, cols], raw.at[k - 2], raw_s, raw_r, dev[k])

    def x_copy(c):
        cols = ranges[c]
        return remote(xs.at[:, cols], xr.at[:, cols], x_s, x_r.at[c - 1], dev[2])

    rows_att = att[...]
    flat = heads * head_dim
    for c, cut in enumerate(cuts):
        piece = jnp.dot(
            rows_att,
            ow_v[:, :, cut].reshape(flat, cut.stop - cut.start),
            preferred_element_type=jnp.float32,
        )
        pbuf[:, :, cut] = piece.astype(jnp.bfloat16).reshape(group, rows, cut.stop - cut.start)
        if c == 0:
            raw_copy(2).start()
            raw_copy(3).start()
        else:
            pair_copy(c).start()
        near_copy(c).start()
    for c in range(1, len(cuts)):
        pair_copy(c).wait_recv()
        cut = cuts[c]
        xs[:, cut] = (
            pbuf[slot[2], :, cut].astype(jnp.float32) + dbuf[1, :, cut].astype(jnp.float32)
        ).astype(jnp.bfloat16)
        x_copy(c).start()

    ncrecv[slot[0]] = ncbuf[slot[0]]
    three = ncrecv.at[pl.ds(0, group - 1)]
    remote(three, three, nc_s, nc_r, dev[1]).wait_recv()
    landed = ncrecv[...].reshape(group * heads, rows, 2 * head_dim)
    nc_out[...] = jnp.transpose(landed, (1, 0, 2))

    sent = st_t.at[pl.ds(0, (group - 1) * heads)]
    remote(sent, sent, st_send, st_recv.at[0], dev[1]).wait_send()
    remote(three, three, nc_s, nc_r, dev[1]).wait_send()
    for sem in (na_s, nb_s, nr_s):
        remote(beside, beside, sem, na_r, dev[1]).wait_send()
    for q in range(patches):
        whole = stale_all.at[q]

        @pl.when(has_right & (q <= p))
        def _():
            remote(whole, whole, zs_r.at[q], z_recv.at[q, 0], {"patch": p + 1}).wait_send()

        @pl.when(has_left & (q >= p))
        def _():
            remote(whole, whole, zs_l.at[q], z_recv.at[q, 0], {"patch": p - 1}).wait_send()

    near = dbuf.at[0]
    remote(near, near, d_s, d_r, dev[1]).wait_recv()
    remote(raw, raw, raw_s, raw_r, dev[2]).wait_recv()
    for c, cut in enumerate(cuts):
        total = pbuf[slot[0], :, cut].astype(jnp.float32) + dbuf[0, :, cut].astype(jnp.float32)
        if c == 0:
            total = total + raw[0].astype(jnp.float32) + raw[1].astype(jnp.float32)
        else:
            x_copy(c).wait_recv()
            total = total + xr[:, cut].astype(jnp.float32)
        upd[:, cut] = (mod[2:3, cut] * total).astype(jnp.bfloat16)
    remote(near, near, d_s, d_r, dev[1]).wait_send()
    remote(raw, raw, raw_s, raw_r, dev[2]).wait_send()
    rest = pl.ds(cuts[1].start, width - cuts[1].start)
    remote(dbuf.at[1, :, rest], dbuf.at[1, :, rest], e_s, e_r.at[0], dev[1]).wait_send()
    remote(xs.at[:, rest], xs.at[:, rest], x_s, x_r.at[0], dev[2]).wait_send()


def store_kernel(upd, cache, upd_out, cache_out, sems):
    first = pltpu.make_async_copy(upd, upd_out, sems.at[0])
    second = pltpu.make_async_copy(cache, cache_out, sems.at[1])
    first.start()
    second.start()
    first.wait()
    second.wait()


def fused_device(
    patches, tokens, modulation, in_weight, query_gain, key_gain, out_weight, stale_cache, lengths
):
    rows, width = tokens.shape
    heads, head_dim = out_weight.shape[:2]
    group = 4
    all_heads = stale_cache.shape[1]
    patch_tok = rows * group
    bf, f32 = jnp.bfloat16, jnp.float32
    raw_cols = OUT_SPLIT[0] * (width // sum(OUT_SPLIT))
    later = len(OUT_SPLIT) - 1
    vm = pl.BlockSpec(memory_space=pltpu.VMEM)
    dma = pltpu.SemaphoreType.DMA
    upd, cache = pl.pallas_call(
        functools.partial(fused_kernel, patches=patches),
        out_shape=(
            jax.ShapeDtypeStruct((rows, width), bf),
            jax.ShapeDtypeStruct((rows, all_heads, 2 * head_dim), bf),
        ),
        in_specs=[pl.BlockSpec(memory_space=pltpu.HBM)] * 8,
        out_specs=(vm, vm),
        scratch_shapes=[
            pltpu.VMEM(tokens.shape, bf),
            pltpu.VMEM(modulation.shape, f32),
            pltpu.VMEM((1, head_dim), f32),
            pltpu.VMEM((1, head_dim), f32),
            pltpu.SMEM(lengths.shape, jnp.int32),
            pltpu.VMEM(stale_cache.shape, bf),
            pltpu.VMEM(in_weight.shape, bf),
            pltpu.VMEM((width, heads * 3 * head_dim), bf),
            pltpu.VMEM(out_weight.shape, bf),
            pltpu.VMEM((all_heads, rows, 2 * head_dim), bf),
            pltpu.VMEM((group, rows, width), bf),
            pltpu.VMEM((patch_tok, heads * 3 * head_dim), f32),
            pltpu.VMEM((patches, group, heads, rows, 2 * head_dim), bf),
            pltpu.VMEM((group, heads, rows, 2 * head_dim), bf),
            pltpu.VMEM((group, heads, rows, 2 * head_dim), bf),
            pltpu.VMEM((heads, patch_tok, head_dim), bf),
            pltpu.VMEM((heads, patch_tok, 1), f32),
            pltpu.VMEM((heads, patch_tok, 1), f32),
            pltpu.VMEM((heads, patch_tok, head_dim), f32),
            pltpu.VMEM((patch_tok, heads * head_dim), bf),
            pltpu.VMEM((group, rows, width), bf),
            pltpu.VMEM((2, rows, width), bf),
            pltpu.VMEM((2, rows, raw_cols), bf),
            pltpu.VMEM((rows, width), bf),
            pltpu.VMEM((rows, width), bf),
            dma((6,)), dma((K_CHUNKS,)), dma, dma, dma((3,)),
            dma((patches,)), dma((patches,)), dma((patches, 4)),
            dma, dma, dma, dma, dma((K_CHUNKS,)), dma((K_CHUNKS,)), dma, dma,
            dma, dma, dma, dma((later,)), dma, dma, dma, dma((later,)),
        ],
        compiler_params=pltpu.CompilerParams(
            collective_id=0, has_side_effects=True, vmem_limit_bytes=48 * 1024 * 1024
        ),
    )(
        *[
            pltpu.with_memory_space_constraint(operand, pltpu.HBM)
            for operand in (
                tokens, modulation, query_gain.reshape(1, -1), key_gain.reshape(1, -1), lengths,
                stale_cache, in_weight, out_weight,
            )
        ]
    )
    return pl.pallas_call(
        store_kernel,
        out_shape=(
            jax.ShapeDtypeStruct(upd.shape, upd.dtype),
            jax.ShapeDtypeStruct(cache.shape, cache.dtype),
        ),
        in_specs=[vm, vm],
        out_specs=[pl.BlockSpec(memory_space=pltpu.HBM)] * 2,
        scratch_shapes=[dma((2,))],
        compiler_params=pltpu.CompilerParams(vmem_limit_bytes=4 * 1024 * 1024),
    )(upd, cache)


def choose(
    patches, group_shape, tokens, modulation, in_weight, query_gain, key_gain, out_weight,
    stale_cache, lengths,
):
    rows, width = tokens.shape
    heads, head_dim = out_weight.shape[:2]
    kv_bytes = patches * 4 * heads * rows * 4 * head_dim
    weight_bytes = 2 * (in_weight.size + out_weight.size)
    fits = (
        group_shape == (2, 2)
        and rows % 16 == 0
        and head_dim % 128 == 0
        and width % (128 * K_CHUNKS) == 0
        and width % (128 * sum(OUT_SPLIT)) == 0
        and width % (TURN * K_CHUNKS) == 0
        and patches > 1
        and rows * 4 * patches <= 1024
        and kv_bytes + weight_bytes <= 24 * 1024 * 1024
    )
    args = (
        tokens, modulation, in_weight, query_gain, key_gain, out_weight, stale_cache, lengths
    )
    return fused_device(patches, *args) if fits else per_device(*args)


def solution(mesh):
    return jax.shard_map(
        functools.partial(
            choose, mesh.shape["patch"], (mesh.shape["head"], mesh.shape["rep"])
        ),
        mesh=mesh,
        in_specs=(
            P(("clip", "patch", "head", "rep"), None),
            P(),
            P(None, ("head", "rep"), None),
            P(),
            P(),
            P(("head", "rep"), None, None),
            P(("clip", "patch", "head", "rep"), None, None),
            P("clip"),
        ),
        out_specs=(
            P(("clip", "patch", "head", "rep"), None),
            P(("clip", "patch", "head", "rep"), None, None),
        ),
        check_vma=False,
    )
```

```python
import functools
import math

import jax
import jax.numpy as jnp
from jax import lax
from jax.experimental import pallas as pl
from jax.experimental.pallas import tpu as pltpu
from jax.sharding import PartitionSpec as P

EPSILON = 1e-06
NEGATIVE = -1e30
key_block = 512


def normalize_rows(values):
    average = jnp.mean(values, axis=-1, keepdims=True)
    centred = values - average
    variance = jnp.mean(centred * centred, axis=-1, keepdims=True)
    return centred * lax.rsqrt(variance + EPSILON)


def rms_gain(values, gain):
    return values * lax.rsqrt(jnp.mean(values * values, axis=-1, keepdims=True) + EPSILON) * gain


def project(normed, in_weight, query_gain, key_gain):
    row_count = normed.shape[0]
    head_count = in_weight.shape[1]
    triple = in_weight.shape[2]
    head_dim = triple // 3
    flat_weight = in_weight.reshape(in_weight.shape[0], head_count * triple)
    projected = jnp.dot(normed, flat_weight, preferred_element_type=jnp.float32).reshape(
        row_count, head_count, triple
    )
    queries = rms_gain(projected[..., :head_dim], query_gain)
    fresh_keys = rms_gain(projected[..., head_dim : 2 * head_dim], key_gain)
    return jnp.concatenate([queries, fresh_keys, projected[..., 2 * head_dim :]], axis=-1).astype(
        jnp.bfloat16
    )


def lookup(lengths, patch_of):
    patch_ids = jnp.arange(lengths.shape[0], dtype=jnp.int32)
    return jnp.sum(jnp.where(patch_of[:, None] == patch_ids[None, :], lengths[None, :], 0), axis=1)


def attend(running, queries, key_rows, usable):
    head_dim = queries.shape[-1]
    row_max, denominator, weighted = running
    scores = jnp.einsum(
        "qhd,khd->qhk", queries, key_rows[..., :head_dim], preferred_element_type=jnp.float32
    )
    scores = scores * (1.0 / math.sqrt(head_dim))
    key_mask = usable[None, None, :]
    scores = jnp.where(key_mask, scores, NEGATIVE)
    new_max = jnp.maximum(row_max, jnp.max(scores, axis=-1))
    weights = jnp.where(key_mask, jnp.exp(scores - new_max[..., None]), 0.0)
    factor = jnp.exp(row_max - new_max)
    denominator = denominator * factor + jnp.sum(weights, axis=-1)
    weighted = weighted * factor[..., None] + jnp.einsum(
        "qhk,khd->qhd",
        weights.astype(jnp.bfloat16),
        key_rows[..., head_dim:],
        preferred_element_type=jnp.float32,
    )
    return (new_max, denominator, weighted)


def attend_blocks(running, queries, key_rows, usable):
    key_count = key_rows.shape[0]
    if key_count > key_block and key_count % key_block == 0:
        shaped = key_rows.reshape((key_count // key_block, key_block) + key_rows.shape[1:])
        usable_rows = usable.reshape(key_count // key_block, key_block)

        def step_block(current, operands):
            return (attend(current, queries, operands[0], operands[1]), None)

        running, _ = lax.scan(step_block, running, (shaped, usable_rows))
        return running
    return attend(running, queries, key_rows, usable)


def per_device(
    tokens, modulation, in_weight, query_gain, key_gain, out_weight, stale_cache, lengths
):
    heads_dev = in_weight.shape[1]
    head_dim = query_gain.shape[0]
    normed = (
        normalize_rows(tokens.astype(jnp.float32)) * (1.0 + modulation[1]) + modulation[0]
    ).astype(jnp.bfloat16)
    fresh = project(
        lax.all_gather(normed, ("head", "rep"), axis=0, tiled=True), in_weight, query_gain, key_gain
    )
    queries = fresh[..., :head_dim]
    own_rows = fresh[..., head_dim:]
    new_cache = lax.all_to_all(own_rows, ("head", "rep"), split_axis=0, concat_axis=1, tiled=True)
    patch_tok = fresh.shape[0]
    own_patch = lax.axis_index("patch")
    own_length = lookup(lengths, jnp.full((1,), own_patch, jnp.int32))[0]
    running = (
        jnp.full((patch_tok, heads_dev), NEGATIVE, jnp.float32),
        jnp.zeros((patch_tok, heads_dev), jnp.float32),
        jnp.zeros((patch_tok, heads_dev, head_dim), jnp.float32),
    )
    running = attend_blocks(
        running, queries, own_rows, jnp.arange(patch_tok, dtype=jnp.int32) < own_length
    )
    stale_heads = lax.all_to_all(
        stale_cache, ("head", "rep"), split_axis=1, concat_axis=0, tiled=True
    )
    shard_part = lax.all_gather(stale_heads, "patch", axis=0, tiled=True)
    key_index = jnp.arange(shard_part.shape[0], dtype=jnp.int32)
    patch_of = key_index // patch_tok
    position = key_index % patch_tok
    usable = (position < lookup(lengths, patch_of)) & (patch_of != own_patch)
    running = attend_blocks(running, queries, shard_part, usable)
    attended = (running[2] / running[1][..., None]).astype(jnp.bfloat16)
    flat_rows = attended.reshape(patch_tok, heads_dev * head_dim)
    flat_weight = out_weight.reshape(heads_dev * head_dim, out_weight.shape[2])
    attention = lax.psum_scatter(
        jnp.dot(flat_rows, flat_weight, preferred_element_type=jnp.float32).astype(jnp.bfloat16),
        ("head", "rep"),
        scatter_dimension=0,
        tiled=True,
    ).astype(jnp.float32)
    update = (modulation[2] * attention).astype(jnp.bfloat16)
    return (update, new_cache)


MESH = pl.DeviceIdType.MESH
K_CHUNKS = 4
OUT_SPLIT = (3, 4, 5, 6, 6)
TURN = 64
SHIP = 1
RELAYS = (1, 2, 4, 5, 6, 6, 7)


def nearest(p, patches, i):
    place = 0
    for own in range(patches):
        others = sorted((q for q in range(patches) if q != own), key=lambda q: (abs(q - own), q))
        place = place + (p == own).astype(jnp.int32) * others[i]
    return place


def fused_kernel(
    tok_hbm, mod_hbm, qg_hbm, kg_hbm, lens_hbm, st_hbm, w_hbm, ow_hbm, upd, nc_out,
    tok, mod, qg, kg, lens, st,
    w_raw, w_v, ow_v, st_t, normed_all, acc, stale_all, ncbuf, ncrecv,
    qbuf, top_v, den_v, out_v, att, pbuf, dbuf, raw, xs, xr,
    guest_q, guest_o, guest_n, home_o, home_n,
    in_sem, w_sem, ow_sem, st_send, st_recv, zs_r, zs_l, z_recv,
    na_s, nb_s, nr_s, na_r, nb_r, nr_r, nc_s, nc_r,
    d_s, d_r, e_s, e_r, raw_s, raw_r, x_s, x_r, gq_s, gq_r, go_s, go_r, gn_s, gn_r,
    *, patches,
):
    p = lax.axis_index("patch")
    h = lax.axis_index("head")
    r = lax.axis_index("rep")
    heads = ow_hbm.shape[0]
    head_dim = ow_hbm.shape[1]
    rows, width = tok.shape
    triple = 3 * head_dim
    kc = width // K_CHUNKS
    group = 4
    patch_tok = group * rows
    coords = [(h, r), (h, 1 - r), (1 - h, r), (1 - h, 1 - r)]
    slot = [a * 2 + b for a, b in coords]
    dev = [{"head": a, "rep": b} for a, b in coords]

    def remote(src, dst, ss, rs, to):
        return pltpu.make_async_remote_copy(
            src_ref=src, dst_ref=dst, send_sem=ss, recv_sem=rs, device_id=to, device_id_type=MESH
        )

    loads = [
        pltpu.make_async_copy(src, dst, in_sem.at[i])
        for i, (src, dst) in enumerate(
            [(st_hbm, st), (tok_hbm, tok), (mod_hbm, mod), (qg_hbm, qg), (kg_hbm, kg), (lens_hbm, lens)]
        )
    ]
    for load in loads:
        load.start()

    has_right = p + 1 < patches
    has_left = p > 0
    barrier = pltpu.get_barrier_semaphore()
    for k in (1, 2, 3):
        pl.semaphore_signal(barrier, inc=1, device_id=dev[k], device_id_type=MESH)

    @pl.when(has_right)
    def _():
        pl.semaphore_signal(barrier, inc=1, device_id={"patch": p + 1}, device_id_type=MESH)

    @pl.when(has_left)
    def _():
        pl.semaphore_signal(barrier, inc=1, device_id={"patch": p - 1}, device_id_type=MESH)

    def w_copy(c):
        return pltpu.make_async_copy(
            w_hbm.at[pl.ds(c * kc, kc)], w_raw.at[pl.ds(c * kc, kc)], w_sem.at[c]
        )

    def w_turn(c):
        w_copy(c).wait()

        @pl.loop(0, kc // TURN)
        def _(i):
            at = pl.multiple_of(c * kc + i * TURN, TURN)
            turned = jnp.transpose(w_raw[pl.ds(at, TURN)], (1, 0, 2))
            for j in range(heads):
                w_v[pl.ds(at, TURN), j * triple : (j + 1) * triple] = turned[j]

    for c in range(K_CHUNKS):
        w_copy(c).start()
    ow_copy = pltpu.make_async_copy(ow_hbm, ow_v, ow_sem)
    ow_copy.start()

    loads[0].wait()
    st_t[...] = jnp.transpose(st[...], (1, 0, 2))
    stale_all[p, slot[0], 0:SHIP] = st_t[pl.ds(slot[0] * heads, SHIP)]

    pl.semaphore_wait(barrier, 3 + has_right.astype(jnp.int32) + has_left.astype(jnp.int32))

    def stale_part(k):
        return st_t.at[pl.ds(slot[k] * heads, heads)]

    def stale_copy(k):
        return remote(
            stale_part(k), stale_all.at[p, slot[0]], st_send, st_recv.at[k - 1], dev[k]
        )

    def stale_arrival(k):
        place = stale_all.at[p, slot[k]]
        remote(place, place, st_send, st_recv.at[k - 1], dev[k]).wait_recv()

    first_end, last_end = p == 0, p == patches - 1
    to_last, to_first = p == patches - 2, p == 1

    def z_copy(q, k, right, outer, own=False):
        keep = SHIP if outer else 0
        place = stale_all.at[q, slot[k], pl.ds(keep, heads - keep)]
        src = st_t.at[pl.ds(slot[0] * heads + keep, heads - keep)] if own else place
        if right:
            return remote(src, place, zs_r.at[q], z_recv.at[q, k], {"patch": p + 1})
        return remote(src, place, zs_l.at[q], z_recv.at[q, k], {"patch": p - 1})

    def z_send(q, k, right, own=False):
        edge = to_last if right else to_first
        inside = (p < patches - 2) if right else (p > 1)

        @pl.when(edge)
        def _():
            z_copy(q, k, right, True, own).start()

        @pl.when(inside)
        def _():
            z_copy(q, k, right, False, own).start()

    def z_own(k):
        z_send(p, k, True, k == 0)
        z_send(p, k, False, k == 0)

    def z_relay(d, k):
        @pl.when((p - d >= 0) & (p < patches - 1))
        def _():
            z_copy(p - d, k, False, False).wait_recv()
            z_send(p - d, k, True)

        @pl.when((p + d < patches) & (p > 0))
        def _():
            z_copy(p + d, k, True, False).wait_recv()
            z_send(p + d, k, False)

    def end_arrivals(distances):
        for d in distances:
            for k in range(group):

                @pl.when((p - d >= 0) & last_end)
                def _():
                    z_copy(p - d, k, False, True).wait_recv()

                @pl.when((p + d < patches) & first_end)
                def _():
                    z_copy(p + d, k, True, True).wait_recv()

    def chunk(k, c):
        return normed_all.at[slot[k], :, pl.ds(c * kc, kc)]

    def feature_across(c):
        return remote(chunk(0, c), chunk(0, c), nb_s, nb_r.at[c], dev[2])

    def feature_beside():
        place = normed_all.at[slot[0]]
        return remote(place, place, na_s, na_r, dev[1])

    def feature_relay(c):
        return remote(chunk(2, c), chunk(2, c), nr_s, nr_r.at[c], dev[1])

    def feature_pass(c):
        remote(chunk(2, c), chunk(2, c), nb_s, nb_r.at[c], dev[2]).wait_recv()
        feature_relay(c).start()

    relays = [(1, 0), (1, 1), (1, 2), (2, 0), (2, 1), (1, 3), (2, 2), (2, 3)]
    relays += [(d, k) for d in range(3, patches - 1) for k in range(group)]
    done = [0]

    def relay_to(count):
        for d, k in relays[done[0] : count]:
            z_relay(d, k)
        done[0] = max(done[0], count)

    z_own(0)
    for k in (2, 3, 1):
        stale_copy(k).start()
    loads[1].wait()
    loads[2].wait()
    values = tok[...].astype(jnp.float32)
    normed = (normalize_rows(values) * (1.0 + mod[1:2, :]) + mod[0:1, :]).astype(jnp.bfloat16)
    normed_all[slot[0]] = normed
    for c in range(K_CHUNKS):
        feature_across(c).start()
    feature_beside().start()
    stale_arrival(1)
    z_own(1)
    w_turn(0)
    w_turn(1)
    relay_to(RELAYS[0])
    stale_arrival(2)
    z_own(2)
    w_turn(2)
    relay_to(RELAYS[1])
    stale_arrival(3)
    z_own(3)
    for c in range(3, K_CHUNKS):
        w_turn(c)
    feature_pass(0)
    beside = normed_all.at[slot[1]]
    remote(beside, beside, na_s, na_r, dev[1]).wait_recv()
    for c in range(K_CHUNKS):
        if c + 1 < K_CHUNKS:
            feature_pass(c + 1)
        remote(chunk(3, c), chunk(3, c), nr_s, nr_r.at[c], dev[1]).wait_recv()
        part = normed_all[:, :, c * kc : (c + 1) * kc].reshape(patch_tok, kc)
        product = jnp.dot(
            part, w_v[c * kc : (c + 1) * kc, :], preferred_element_type=jnp.float32
        )
        if c == 0:
            acc[...] = product
        else:
            acc[...] += product
        relay_to(RELAYS[2 + c])

    for load in loads[3:]:
        load.wait()
    q_gain = qg[...]
    k_gain = kg[...]
    def query_of(j):
        base = j * triple
        qbuf[j] = rms_gain(acc[:, base : base + head_dim], q_gain).astype(jnp.bfloat16)

    for j in range(SHIP):
        query_of(j)
    leaving = qbuf.at[pl.ds(0, SHIP)]

    def guest_copy(step):
        return remote(leaving, guest_q, gq_s, gq_r, {"patch": p + step})

    @pl.when(first_end)
    def _():
        guest_copy(1).start()

    @pl.when(last_end)
    def _():
        guest_copy(-1).start()

    for j in range(heads):
        base = j * triple
        keys = rms_gain(acc[:, base + head_dim : base + 2 * head_dim], k_gain).astype(jnp.bfloat16)
        ncbuf[:, j, :, :head_dim] = keys.reshape(group, rows, head_dim)
        ncbuf[:, j, :, head_dim:] = (
            acc[:, base + 2 * head_dim : base + triple]
            .astype(jnp.bfloat16)
            .reshape(group, rows, head_dim)
        )
        if j >= SHIP:
            query_of(j)

    def cache_copy(k):
        return remote(
            ncbuf.at[slot[k]], ncrecv.at[slot[0]], nc_s, nc_r, dev[k]
        )

    for k in (2, 3, 1):
        cache_copy(k).start()
    relay_to(RELAYS[2 + K_CHUNKS])
    scale = 1.0 / math.sqrt(head_dim)
    columns = lax.broadcasted_iota(jnp.int32, (1, patch_tok), 1)
    contract = (((1,), (1,)), ((), ()))

    def attend_part(sources, used, asking, first, finish):
        masks = [columns < live for _, live in sources]
        scores = {
            j: [
                lax.dot_general(
                    asking[j],
                    source[:, j, :, :head_dim].reshape(patch_tok, head_dim),
                    contract,
                    preferred_element_type=jnp.float32,
                )
                for source, _ in sources
            ]
            for j in used
        }
        scores = {
            j: [jnp.where(mask, part * scale, NEGATIVE) for part, mask in zip(scores[j], masks)]
            for j in used
        }
        tops = {
            j: functools.reduce(
                jnp.maximum, [jnp.max(part, axis=1, keepdims=True) for part in scores[j]]
            )
            for j in used
        }
        if not first:
            before = {j: top_v[j] for j in used}
            tops = {j: jnp.maximum(before[j], tops[j]) for j in used}
            factor = {j: jnp.exp(before[j] - tops[j]) for j in used}
        weights = {
            j: [
                jnp.where(mask, jnp.exp(part - tops[j]), 0.0)
                for part, mask in zip(scores[j], masks)
            ]
            for j in used
        }
        mixed = {
            j: sum(
                jnp.dot(
                    part.astype(jnp.bfloat16),
                    source[:, j, :, head_dim:].reshape(patch_tok, head_dim),
                    preferred_element_type=jnp.float32,
                )
                for part, (source, _) in zip(weights[j], sources)
            )
            for j in used
        }
        total = {
            j: sum(jnp.sum(part, axis=1, keepdims=True) for part in weights[j]) for j in used
        }
        if not first:
            total = {j: total[j] + den_v[j] * factor[j] for j in used}
            mixed = {j: mixed[j] + out_v[j] * factor[j] for j in used}
        for j in used:
            finish(j, tops[j], total[j], mixed[j])

    def keep_part(j, top, total, mixed):
        top_v[j] = top
        den_v[j] = total
        out_v[j] = mixed

    def put_result(j, top, total, mixed):
        att[:, j * head_dim : (j + 1) * head_dim] = (mixed / total).astype(jnp.bfloat16)

    def other(owner, i):
        q = nearest(owner, patches, i)
        return stale_all.at[q], lens[q]

    every = list(range(heads))
    kept = list(range(SHIP, heads))
    shipped = list(range(SHIP))
    is_end = first_end | last_end
    is_host = to_first | to_last
    lane = lax.broadcasted_iota(jnp.int32, (patch_tok, head_dim), 1)
    home = to_last.astype(jnp.int32) * (patches - 1)

    def back_copies(to):
        return (
            remote(guest_o, home_o, go_s, go_r, {"patch": to}),
            remote(guest_n, home_n, gn_s, gn_r, {"patch": to}),
        )

    def put_guest(j, top, total, mixed):
        guest_o[j] = (mixed / total).astype(jnp.bfloat16)
        notes = jnp.where(lane == 0, top, jnp.where(lane == 1, total, 0.0))
        guest_n[j] = jnp.transpose(notes, (1, 0))[0:8]

    attend_part([(ncbuf, lens[p])], every, qbuf, True, keep_part)
    relay_to(len(relays))

    @pl.when(is_host)
    def _():
        guest_copy(0).wait_recv()
        sources = [other(home, i) for i in range(patches - 1)]
        attend_part(sources, shipped, guest_q, True, put_guest)
        for back in back_copies(home):
            back.start()


    @pl.when(p * (patches - 1 - p) > 0)
    def _():
        sources = [other(p, i) for i in range(patches - 1)]
        attend_part(sources, every, qbuf, False, put_result)

    @pl.when(is_end)
    def _():
        end_arrivals(range(1, patches - 1))
        sources = [other(p, i) for i in range(patches - 2)]
        attend_part(sources, kept, qbuf, False, keep_part)

    end_arrivals([patches - 1])

    @pl.when(is_end)
    def _():
        attend_part([other(p, patches - 2)], kept, qbuf, False, put_result)


    @pl.when(is_end)
    def _():
        for back in back_copies(home):
            back.wait_recv()
        for j in shipped:
            notes = jnp.concatenate(
                [home_n[j], jnp.zeros((patch_tok - 8, patch_tok), jnp.float32)], axis=0
            )
            notes = jnp.transpose(notes, (1, 0))
            top, total = notes[:, 0:1], notes[:, 1:2]
            highest = jnp.maximum(top, top_v[j])
            away = total * jnp.exp(top - highest)
            here = jnp.exp(top_v[j] - highest)
            mixed = home_o[j].astype(jnp.float32) * away + out_v[j] * here
            put_result(j, highest, away + den_v[j] * here, mixed)

    ow_copy.wait()

    cuts = []
    for units in OUT_SPLIT:
        begin = cuts[-1].stop if cuts else 0
        cuts.append(slice(begin, begin + units * (width // sum(OUT_SPLIT))))
    ranges = [pl.ds(cut.start, cut.stop - cut.start) for cut in cuts]

    def near_copy(c):
        cols = ranges[c]
        return remote(pbuf.at[slot[1], :, cols], dbuf.at[0, :, cols], d_s, d_r, dev[1])

    def pair_copy(c):
        cols = ranges[c]
        return remote(pbuf.at[slot[3], :, cols], dbuf.at[1, :, cols], e_s, e_r.at[c - 1], dev[1])

    def raw_copy(k):
        cols = ranges[0]
        return remote(pbuf.at[slot[k], :, cols], raw.at[k - 2], raw_s, raw_r, dev[k])

    def x_copy(c):
        cols = ranges[c]
        return remote(xs.at[:, cols], xr.at[:, cols], x_s, x_r.at[c - 1], dev[2])

    rows_att = att[...]
    flat = heads * head_dim
    for c, cut in enumerate(cuts):
        piece = jnp.dot(
            rows_att,
            ow_v[:, :, cut].reshape(flat, cut.stop - cut.start),
            preferred_element_type=jnp.float32,
        )
        pbuf[:, :, cut] = piece.astype(jnp.bfloat16).reshape(group, rows, cut.stop - cut.start)
        if c == 0:
            raw_copy(2).start()
            raw_copy(3).start()
        else:
            pair_copy(c).start()
        near_copy(c).start()
    for c in range(1, len(cuts)):
        pair_copy(c).wait_recv()
        cut = cuts[c]
        xs[:, cut] = (
            pbuf[slot[2], :, cut].astype(jnp.float32) + dbuf[1, :, cut].astype(jnp.float32)
        ).astype(jnp.bfloat16)
        x_copy(c).start()

    ncrecv[slot[0]] = ncbuf[slot[0]]
    three = ncrecv.at[pl.ds(0, group - 1)]
    remote(three, three, nc_s, nc_r, dev[1]).wait_recv()
    landed = ncrecv[...].reshape(group * heads, rows, 2 * head_dim)
    nc_out[...] = jnp.transpose(landed, (1, 0, 2))

    sent = st_t.at[pl.ds(0, (group - 1) * heads)]
    remote(sent, sent, st_send, st_recv.at[0], dev[1]).wait_send()
    remote(three, three, nc_s, nc_r, dev[1]).wait_send()
    for sem in (na_s, nb_s, nr_s):
        remote(beside, beside, sem, na_r, dev[1]).wait_send()
    for q in range(patches):
        whole = stale_all.at[q]
        outer = stale_all.at[q, :, pl.ds(SHIP, heads - SHIP)]

        @pl.when((p < patches - 2) & (q <= p))
        def _():
            remote(whole, whole, zs_r.at[q], z_recv.at[q, 0], {"patch": p + 1}).wait_send()

        @pl.when(to_last & (q <= p))
        def _():
            remote(outer, outer, zs_r.at[q], z_recv.at[q, 0], {"patch": p + 1}).wait_send()

        @pl.when((p > 1) & (q >= p))
        def _():
            remote(whole, whole, zs_l.at[q], z_recv.at[q, 0], {"patch": p - 1}).wait_send()

        @pl.when(to_first & (q >= p))
        def _():
            remote(outer, outer, zs_l.at[q], z_recv.at[q, 0], {"patch": p - 1}).wait_send()

    @pl.when(is_end)
    def _():
        guest_copy(0).wait_send()

    @pl.when(is_host)
    def _():
        for back in back_copies(home):
            back.wait_send()

    near = dbuf.at[0]
    remote(near, near, d_s, d_r, dev[1]).wait_recv()
    remote(raw, raw, raw_s, raw_r, dev[2]).wait_recv()
    for c, cut in enumerate(cuts):
        total = pbuf[slot[0], :, cut].astype(jnp.float32) + dbuf[0, :, cut].astype(jnp.float32)
        if c == 0:
            total = total + raw[0].astype(jnp.float32) + raw[1].astype(jnp.float32)
        else:
            x_copy(c).wait_recv()
            total = total + xr[:, cut].astype(jnp.float32)
        upd[:, cut] = (mod[2:3, cut] * total).astype(jnp.bfloat16)
    remote(near, near, d_s, d_r, dev[1]).wait_send()
    remote(raw, raw, raw_s, raw_r, dev[2]).wait_send()
    rest = pl.ds(cuts[1].start, width - cuts[1].start)
    remote(dbuf.at[1, :, rest], dbuf.at[1, :, rest], e_s, e_r.at[0], dev[1]).wait_send()
    remote(xs.at[:, rest], xs.at[:, rest], x_s, x_r.at[0], dev[2]).wait_send()


def store_kernel(upd, cache, upd_out, cache_out, sems):
    first = pltpu.make_async_copy(upd, upd_out, sems.at[0])
    second = pltpu.make_async_copy(cache, cache_out, sems.at[1])
    first.start()
    second.start()
    first.wait()
    second.wait()


def fused_device(
    patches, tokens, modulation, in_weight, query_gain, key_gain, out_weight, stale_cache, lengths
):
    rows, width = tokens.shape
    heads, head_dim = out_weight.shape[:2]
    group = 4
    all_heads = stale_cache.shape[1]
    patch_tok = rows * group
    bf, f32 = jnp.bfloat16, jnp.float32
    raw_cols = OUT_SPLIT[0] * (width // sum(OUT_SPLIT))
    later = len(OUT_SPLIT) - 1
    vm = pl.BlockSpec(memory_space=pltpu.VMEM)
    dma = pltpu.SemaphoreType.DMA
    upd, cache = pl.pallas_call(
        functools.partial(fused_kernel, patches=patches),
        out_shape=(
            jax.ShapeDtypeStruct((rows, width), bf),
            jax.ShapeDtypeStruct((rows, all_heads, 2 * head_dim), bf),
        ),
        in_specs=[pl.BlockSpec(memory_space=pltpu.HBM)] * 8,
        out_specs=(vm, vm),
        scratch_shapes=[
            pltpu.VMEM(tokens.shape, bf),
            pltpu.VMEM(modulation.shape, f32),
            pltpu.VMEM((1, head_dim), f32),
            pltpu.VMEM((1, head_dim), f32),
            pltpu.SMEM(lengths.shape, jnp.int32),
            pltpu.VMEM(stale_cache.shape, bf),
            pltpu.VMEM(in_weight.shape, bf),
            pltpu.VMEM((width, heads * 3 * head_dim), bf),
            pltpu.VMEM(out_weight.shape, bf),
            pltpu.VMEM((all_heads, rows, 2 * head_dim), bf),
            pltpu.VMEM((group, rows, width), bf),
            pltpu.VMEM((patch_tok, heads * 3 * head_dim), f32),
            pltpu.VMEM((patches, group, heads, rows, 2 * head_dim), bf),
            pltpu.VMEM((group, heads, rows, 2 * head_dim), bf),
            pltpu.VMEM((group, heads, rows, 2 * head_dim), bf),
            pltpu.VMEM((heads, patch_tok, head_dim), bf),
            pltpu.VMEM((heads, patch_tok, 1), f32),
            pltpu.VMEM((heads, patch_tok, 1), f32),
            pltpu.VMEM((heads, patch_tok, head_dim), f32),
            pltpu.VMEM((patch_tok, heads * head_dim), bf),
            pltpu.VMEM((group, rows, width), bf),
            pltpu.VMEM((2, rows, width), bf),
            pltpu.VMEM((2, rows, raw_cols), bf),
            pltpu.VMEM((rows, width), bf),
            pltpu.VMEM((rows, width), bf),
            pltpu.VMEM((SHIP, patch_tok, head_dim), bf),
            pltpu.VMEM((SHIP, patch_tok, head_dim), bf),
            pltpu.VMEM((SHIP, 8, patch_tok), f32),
            pltpu.VMEM((SHIP, patch_tok, head_dim), bf),
            pltpu.VMEM((SHIP, 8, patch_tok), f32),
            dma((6,)), dma((K_CHUNKS,)), dma, dma, dma((3,)),
            dma((patches,)), dma((patches,)), dma((patches, 4)),
            dma, dma, dma, dma, dma((K_CHUNKS,)), dma((K_CHUNKS,)), dma, dma,
            dma, dma, dma, dma((later,)), dma, dma, dma, dma((later,)),
            dma, dma, dma, dma, dma, dma,
        ],
        compiler_params=pltpu.CompilerParams(
            collective_id=0, has_side_effects=True, vmem_limit_bytes=48 * 1024 * 1024
        ),
    )(
        *[
            pltpu.with_memory_space_constraint(operand, pltpu.HBM)
            for operand in (
                tokens, modulation, query_gain.reshape(1, -1), key_gain.reshape(1, -1), lengths,
                stale_cache, in_weight, out_weight,
            )
        ]
    )
    return pl.pallas_call(
        store_kernel,
        out_shape=(
            jax.ShapeDtypeStruct(upd.shape, upd.dtype),
            jax.ShapeDtypeStruct(cache.shape, cache.dtype),
        ),
        in_specs=[vm, vm],
        out_specs=[pl.BlockSpec(memory_space=pltpu.HBM)] * 2,
        scratch_shapes=[dma((2,))],
        compiler_params=pltpu.CompilerParams(vmem_limit_bytes=4 * 1024 * 1024),
    )(upd, cache)


def choose(
    patches, group_shape, tokens, modulation, in_weight, query_gain, key_gain, out_weight,
    stale_cache, lengths,
):
    rows, width = tokens.shape
    heads, head_dim = out_weight.shape[:2]
    kv_bytes = patches * 4 * heads * rows * 4 * head_dim
    weight_bytes = 2 * (in_weight.size + out_weight.size)
    fits = (
        group_shape == (2, 2)
        and rows % 16 == 0
        and head_dim % 128 == 0
        and width % (128 * K_CHUNKS) == 0
        and width % (128 * sum(OUT_SPLIT)) == 0
        and width % (TURN * K_CHUNKS) == 0
        and patches > 3
        and heads > SHIP
        and rows * 4 == head_dim
        and rows * 4 * patches <= 1024
        and kv_bytes + weight_bytes <= 24 * 1024 * 1024
    )
    args = (
        tokens, modulation, in_weight, query_gain, key_gain, out_weight, stale_cache, lengths
    )
    return fused_device(patches, *args) if fits else per_device(*args)


def solution(mesh):
    return jax.shard_map(
        functools.partial(
            choose, mesh.shape["patch"], (mesh.shape["head"], mesh.shape["rep"])
        ),
        mesh=mesh,
        in_specs=(
            P(("clip", "patch", "head", "rep"), None),
            P(),
            P(None, ("head", "rep"), None),
            P(),
            P(),
            P(("head", "rep"), None, None),
            P(("clip", "patch", "head", "rep"), None, None),
            P("clip"),
        ),
        out_specs=(
            P(("clip", "patch", "head", "rep"), None),
            P(("clip", "patch", "head", "rep"), None, None),
        ),
        check_vma=False,
    )
```

```python
import functools
import math

import jax
import jax.numpy as jnp
from jax import lax
from jax.experimental import pallas as pl
from jax.experimental.pallas import tpu as pltpu
from jax.sharding import PartitionSpec as P

EPSILON = 1e-06
NEGATIVE = -1e30
key_block = 512


def normalize_rows(values):
    average = jnp.mean(values, axis=-1, keepdims=True)
    centred = values - average
    variance = jnp.mean(centred * centred, axis=-1, keepdims=True)
    return centred * lax.rsqrt(variance + EPSILON)


def rms_gain(values, gain):
    return values * lax.rsqrt(jnp.mean(values * values, axis=-1, keepdims=True) + EPSILON) * gain


def project(normed, in_weight, query_gain, key_gain):
    row_count = normed.shape[0]
    head_count = in_weight.shape[1]
    triple = in_weight.shape[2]
    head_dim = triple // 3
    flat_weight = in_weight.reshape(in_weight.shape[0], head_count * triple)
    projected = jnp.dot(normed, flat_weight, preferred_element_type=jnp.float32).reshape(
        row_count, head_count, triple
    )
    queries = rms_gain(projected[..., :head_dim], query_gain)
    fresh_keys = rms_gain(projected[..., head_dim : 2 * head_dim], key_gain)
    return jnp.concatenate([queries, fresh_keys, projected[..., 2 * head_dim :]], axis=-1).astype(
        jnp.bfloat16
    )


def lookup(lengths, patch_of):
    patch_ids = jnp.arange(lengths.shape[0], dtype=jnp.int32)
    return jnp.sum(jnp.where(patch_of[:, None] == patch_ids[None, :], lengths[None, :], 0), axis=1)


def attend(running, queries, key_rows, usable):
    head_dim = queries.shape[-1]
    row_max, denominator, weighted = running
    scores = jnp.einsum(
        "qhd,khd->qhk", queries, key_rows[..., :head_dim], preferred_element_type=jnp.float32
    )
    scores = scores * (1.0 / math.sqrt(head_dim))
    key_mask = usable[None, None, :]
    scores = jnp.where(key_mask, scores, NEGATIVE)
    new_max = jnp.maximum(row_max, jnp.max(scores, axis=-1))
    weights = jnp.where(key_mask, jnp.exp(scores - new_max[..., None]), 0.0)
    factor = jnp.exp(row_max - new_max)
    denominator = denominator * factor + jnp.sum(weights, axis=-1)
    weighted = weighted * factor[..., None] + jnp.einsum(
        "qhk,khd->qhd",
        weights.astype(jnp.bfloat16),
        key_rows[..., head_dim:],
        preferred_element_type=jnp.float32,
    )
    return (new_max, denominator, weighted)


def attend_blocks(running, queries, key_rows, usable):
    key_count = key_rows.shape[0]
    if key_count > key_block and key_count % key_block == 0:
        shaped = key_rows.reshape((key_count // key_block, key_block) + key_rows.shape[1:])
        usable_rows = usable.reshape(key_count // key_block, key_block)

        def step_block(current, operands):
            return (attend(current, queries, operands[0], operands[1]), None)

        running, _ = lax.scan(step_block, running, (shaped, usable_rows))
        return running
    return attend(running, queries, key_rows, usable)


def per_device(
    tokens, modulation, in_weight, query_gain, key_gain, out_weight, stale_cache, lengths
):
    heads_dev = in_weight.shape[1]
    head_dim = query_gain.shape[0]
    normed = (
        normalize_rows(tokens.astype(jnp.float32)) * (1.0 + modulation[1]) + modulation[0]
    ).astype(jnp.bfloat16)
    fresh = project(
        lax.all_gather(normed, ("head", "rep"), axis=0, tiled=True), in_weight, query_gain, key_gain
    )
    queries = fresh[..., :head_dim]
    own_rows = fresh[..., head_dim:]
    new_cache = lax.all_to_all(own_rows, ("head", "rep"), split_axis=0, concat_axis=1, tiled=True)
    patch_tok = fresh.shape[0]
    own_patch = lax.axis_index("patch")
    own_length = lookup(lengths, jnp.full((1,), own_patch, jnp.int32))[0]
    running = (
        jnp.full((patch_tok, heads_dev), NEGATIVE, jnp.float32),
        jnp.zeros((patch_tok, heads_dev), jnp.float32),
        jnp.zeros((patch_tok, heads_dev, head_dim), jnp.float32),
    )
    running = attend_blocks(
        running, queries, own_rows, jnp.arange(patch_tok, dtype=jnp.int32) < own_length
    )
    stale_heads = lax.all_to_all(
        stale_cache, ("head", "rep"), split_axis=1, concat_axis=0, tiled=True
    )
    shard_part = lax.all_gather(stale_heads, "patch", axis=0, tiled=True)
    key_index = jnp.arange(shard_part.shape[0], dtype=jnp.int32)
    patch_of = key_index // patch_tok
    position = key_index % patch_tok
    usable = (position < lookup(lengths, patch_of)) & (patch_of != own_patch)
    running = attend_blocks(running, queries, shard_part, usable)
    attended = (running[2] / running[1][..., None]).astype(jnp.bfloat16)
    flat_rows = attended.reshape(patch_tok, heads_dev * head_dim)
    flat_weight = out_weight.reshape(heads_dev * head_dim, out_weight.shape[2])
    attention = lax.psum_scatter(
        jnp.dot(flat_rows, flat_weight, preferred_element_type=jnp.float32).astype(jnp.bfloat16),
        ("head", "rep"),
        scatter_dimension=0,
        tiled=True,
    ).astype(jnp.float32)
    update = (modulation[2] * attention).astype(jnp.bfloat16)
    return (update, new_cache)


MESH = pl.DeviceIdType.MESH
K_CHUNKS = 4
OUT_SPLIT = (3, 4, 5, 6, 6)
TURN = 64
SHIP = 1
RELAY_ORDER = ((1, 0), (1, 1), (1, 2), (2, 0), (2, 1), (1, 3), (1, 4), (2, 2), (2, 3), (2, 4))
RELAYS = (1, 2, 4, 5, 7, 7, 8)


def nearest(p, patches, i):
    place = 0
    for own in range(patches):
        others = sorted((q for q in range(patches) if q != own), key=lambda q: (abs(q - own), q))
        place = place + (p == own).astype(jnp.int32) * others[i]
    return place


def fused_kernel(
    tok_hbm, mod_hbm, qg_hbm, kg_hbm, lens_hbm, st_hbm, w_hbm, ow_hbm, upd, nc_out,
    tok, mod, qg, kg, lens, st,
    w_raw, w_v, ow_v, st_t, normed_all, acc, stale_all, ncbuf, ncrecv,
    qbuf, top_v, den_v, out_v, att, pbuf, dbuf, raw, xs, xr,
    guest_q, guest_o, guest_n, home_o, home_n,
    in_sem, w_sem, ow_sem, st_send, st_recv, zs_r, zs_l, z_recv,
    na_s, nb_s, nr_s, na_r, nb_r, nr_r, nc_s, nc_r,
    d_s, d_r, e_s, e_r, raw_s, raw_r, x_s, x_r, far_s, gq_s, gq_r, go_s, go_r, gn_s, gn_r,
    *, patches,
):
    p = lax.axis_index("patch")
    h = lax.axis_index("head")
    r = lax.axis_index("rep")
    heads = ow_hbm.shape[0]
    head_dim = ow_hbm.shape[1]
    rows, width = tok.shape
    triple = 3 * head_dim
    kc = width // K_CHUNKS
    group = 4
    patch_tok = group * rows
    coords = [(h, r), (h, 1 - r), (1 - h, r), (1 - h, 1 - r)]
    slot = [a * 2 + b for a, b in coords]
    dev = [{"head": a, "rep": b} for a, b in coords]

    def remote(src, dst, ss, rs, to):
        return pltpu.make_async_remote_copy(
            src_ref=src, dst_ref=dst, send_sem=ss, recv_sem=rs, device_id=to, device_id_type=MESH
        )

    loads = [
        pltpu.make_async_copy(src, dst, in_sem.at[i])
        for i, (src, dst) in enumerate(
            [(st_hbm, st), (tok_hbm, tok), (mod_hbm, mod), (qg_hbm, qg), (kg_hbm, kg), (lens_hbm, lens)]
        )
    ]
    for load in loads:
        load.start()

    has_right = p + 1 < patches
    has_left = p > 0
    barrier = pltpu.get_barrier_semaphore()
    for k in (1, 2, 3):
        pl.semaphore_signal(barrier, inc=1, device_id=dev[k], device_id_type=MESH)

    @pl.when(has_right)
    def _():
        pl.semaphore_signal(barrier, inc=1, device_id={"patch": p + 1}, device_id_type=MESH)

    @pl.when(has_left)
    def _():
        pl.semaphore_signal(barrier, inc=1, device_id={"patch": p - 1}, device_id_type=MESH)

    def w_copy(c):
        return pltpu.make_async_copy(
            w_hbm.at[pl.ds(c * kc, kc)], w_raw.at[pl.ds(c * kc, kc)], w_sem.at[c]
        )

    def w_turn(c):
        w_copy(c).wait()

        @pl.loop(0, kc // TURN)
        def _(i):
            at = pl.multiple_of(c * kc + i * TURN, TURN)
            turned = jnp.transpose(w_raw[pl.ds(at, TURN)], (1, 0, 2))
            for j in range(heads):
                w_v[pl.ds(at, TURN), j * triple : (j + 1) * triple] = turned[j]

    for c in range(K_CHUNKS):
        w_copy(c).start()
    ow_copy = pltpu.make_async_copy(ow_hbm, ow_v, ow_sem)
    ow_copy.start()

    loads[0].wait()
    st_t[...] = jnp.transpose(st[...], (1, 0, 2))
    stale_all[p, slot[0], 0:SHIP] = st_t[pl.ds(slot[0] * heads, SHIP)]

    pl.semaphore_wait(barrier, 3 + has_right.astype(jnp.int32) + has_left.astype(jnp.int32))

    def stale_part(k):
        return st_t.at[pl.ds(slot[k] * heads, heads)]

    def stale_copy(k):
        return remote(
            stale_part(k), stale_all.at[p, slot[0]], st_send, st_recv.at[k - 1], dev[k]
        )

    def stale_arrival(k):
        place = stale_all.at[p, slot[k]]
        remote(place, place, st_send, st_recv.at[k - 1], dev[k]).wait_recv()

    first_end, last_end = p == 0, p == patches - 1
    to_last, to_first = p == patches - 2, p == 1

    def landing(q, step, k):
        return z_recv.at[(q - p - step + patches) % patches - 1, k]

    def z_copy(q, k, right, outer, own=False):
        begin = SHIP if outer or k == 4 else 0
        end = SHIP if k == 3 else heads
        place = stale_all.at[q, slot[min(k, 3)], pl.ds(begin, end - begin)]
        src = place
        if own and k == 0:
            src = st_t.at[pl.ds(slot[0] * heads + begin, end - begin)]
        if right:
            return remote(src, place, zs_r.at[q], landing(q, 1, k), {"patch": p + 1})
        return remote(src, place, zs_l.at[q], landing(q, -1, k), {"patch": p - 1})

    def z_landed(q, k, outer):
        begin = SHIP if outer or k == 4 else 0
        end = SHIP if k == 3 else heads
        place = stale_all.at[q, slot[min(k, 3)], pl.ds(begin, end - begin)]
        remote(place, place, far_s, landing(q, 0, k), dev[1]).wait_recv()

    def z_send(q, k, right, own=False):
        if k != 3:

            @pl.when(to_last if right else to_first)
            def _():
                z_copy(q, k, right, True, own).start()

        @pl.when((p < patches - 2) if right else (p > 1))
        def _():
            z_copy(q, k, right, False, own).start()

    def z_own(k):
        z_send(p, k, True, k == 0)
        z_send(p, k, False, k == 0)

    def z_straight(right):
        q = 0 if right else patches - 1
        place = stale_all.at[q, slot[3], pl.ds(SHIP, heads - SHIP)]
        step = 2 if right else -2
        return remote(place, place, far_s, landing(q, step, 4), {"patch": p + step})

    def z_relay(d, k):
        @pl.when((p - d >= 0) & (p < patches - 1))
        def _():
            z_landed(p - d, k, False)
            if (d, k) != (2, 4):
                z_send(p - d, k, True)

        @pl.when((p + d < patches) & (p > 0))
        def _():
            z_landed(p + d, k, False)
            if (d, k) != (2, 4):
                z_send(p + d, k, False)

        if (d, k) == (1, 4):

            @pl.when(to_first)
            def _():
                z_straight(True).start()

            @pl.when(to_last)
            def _():
                z_straight(False).start()

    def end_arrivals(distances):
        for d in distances:
            for k in (0, 1, 2, 4):

                @pl.when((p - d >= 0) & last_end)
                def _():
                    z_landed(p - d, k, True)

                @pl.when((p + d < patches) & first_end)
                def _():
                    z_landed(p + d, k, True)

    def chunk(k, c):
        return normed_all.at[slot[k], :, pl.ds(c * kc, kc)]

    def feature_across(c):
        return remote(chunk(0, c), chunk(0, c), nb_s, nb_r.at[c], dev[2])

    def feature_beside():
        place = normed_all.at[slot[0]]
        return remote(place, place, na_s, na_r, dev[1])

    def feature_relay(c):
        return remote(chunk(2, c), chunk(2, c), nr_s, nr_r.at[c], dev[1])

    def feature_pass(c):
        remote(chunk(2, c), chunk(2, c), nb_s, nb_r.at[c], dev[2]).wait_recv()
        feature_relay(c).start()

    relays = RELAY_ORDER
    done = [0]

    def relay_to(count):
        for d, k in relays[done[0] : count]:
            z_relay(d, k)
        done[0] = max(done[0], count)

    z_own(0)
    for k in (2, 3, 1):
        stale_copy(k).start()
    loads[1].wait()
    loads[2].wait()
    values = tok[...].astype(jnp.float32)
    normed = (normalize_rows(values) * (1.0 + mod[1:2, :]) + mod[0:1, :]).astype(jnp.bfloat16)
    normed_all[slot[0]] = normed
    for c in range(K_CHUNKS):
        feature_across(c).start()
    feature_beside().start()
    stale_arrival(1)
    z_own(1)
    w_turn(0)
    w_turn(1)
    relay_to(RELAYS[0])
    stale_arrival(2)
    z_own(2)
    w_turn(2)
    relay_to(RELAYS[1])
    stale_arrival(3)
    z_own(3)
    z_own(4)
    for c in range(3, K_CHUNKS):
        w_turn(c)
    feature_pass(0)
    beside = normed_all.at[slot[1]]
    remote(beside, beside, na_s, na_r, dev[1]).wait_recv()
    for c in range(K_CHUNKS):
        if c + 1 < K_CHUNKS:
            feature_pass(c + 1)
        remote(chunk(3, c), chunk(3, c), nr_s, nr_r.at[c], dev[1]).wait_recv()
        part = normed_all[:, :, c * kc : (c + 1) * kc].reshape(patch_tok, kc)
        product = jnp.dot(
            part, w_v[c * kc : (c + 1) * kc, :], preferred_element_type=jnp.float32
        )
        if c == 0:
            acc[...] = product
        else:
            acc[...] += product
        relay_to(RELAYS[2 + c])

    for load in loads[3:]:
        load.wait()
    q_gain = qg[...]
    k_gain = kg[...]
    def query_of(j):
        base = j * triple
        qbuf[j] = rms_gain(acc[:, base : base + head_dim], q_gain).astype(jnp.bfloat16)

    for j in range(SHIP):
        query_of(j)
    leaving = qbuf.at[pl.ds(0, SHIP)]

    def guest_copy(step):
        return remote(leaving, guest_q, gq_s, gq_r, {"patch": p + step})

    @pl.when(first_end)
    def _():
        guest_copy(1).start()

    @pl.when(last_end)
    def _():
        guest_copy(-1).start()

    for j in range(heads):
        base = j * triple
        keys = rms_gain(acc[:, base + head_dim : base + 2 * head_dim], k_gain).astype(jnp.bfloat16)
        ncbuf[:, j, :, :head_dim] = keys.reshape(group, rows, head_dim)
        ncbuf[:, j, :, head_dim:] = (
            acc[:, base + 2 * head_dim : base + triple]
            .astype(jnp.bfloat16)
            .reshape(group, rows, head_dim)
        )
        if j >= SHIP:
            query_of(j)

    def cache_copy(k):
        return remote(
            ncbuf.at[slot[k]], ncrecv.at[slot[0]], nc_s, nc_r, dev[k]
        )

    for k in (2, 3, 1):
        cache_copy(k).start()
    relay_to(RELAYS[2 + K_CHUNKS])
    scale = 1.0 / math.sqrt(head_dim)
    columns = lax.broadcasted_iota(jnp.int32, (1, patch_tok), 1)
    contract = (((1,), (1,)), ((), ()))

    def attend_part(sources, used, asking, first, finish):
        masks = [columns < live for _, live in sources]
        scores = {
            j: [
                lax.dot_general(
                    asking[j],
                    source[:, j, :, :head_dim].reshape(patch_tok, head_dim),
                    contract,
                    preferred_element_type=jnp.float32,
                )
                for source, _ in sources
            ]
            for j in used
        }
        scores = {
            j: [jnp.where(mask, part * scale, NEGATIVE) for part, mask in zip(scores[j], masks)]
            for j in used
        }
        tops = {
            j: functools.reduce(
                jnp.maximum, [jnp.max(part, axis=1, keepdims=True) for part in scores[j]]
            )
            for j in used
        }
        if not first:
            before = {j: top_v[j] for j in used}
            tops = {j: jnp.maximum(before[j], tops[j]) for j in used}
            factor = {j: jnp.exp(before[j] - tops[j]) for j in used}
        weights = {
            j: [
                jnp.where(mask, jnp.exp(part - tops[j]), 0.0)
                for part, mask in zip(scores[j], masks)
            ]
            for j in used
        }
        mixed = {
            j: sum(
                jnp.dot(
                    part.astype(jnp.bfloat16),
                    source[:, j, :, head_dim:].reshape(patch_tok, head_dim),
                    preferred_element_type=jnp.float32,
                )
                for part, (source, _) in zip(weights[j], sources)
            )
            for j in used
        }
        total = {
            j: sum(jnp.sum(part, axis=1, keepdims=True) for part in weights[j]) for j in used
        }
        if not first:
            total = {j: total[j] + den_v[j] * factor[j] for j in used}
            mixed = {j: mixed[j] + out_v[j] * factor[j] for j in used}
        for j in used:
            finish(j, tops[j], total[j], mixed[j])

    def keep_part(j, top, total, mixed):
        top_v[j] = top
        den_v[j] = total
        out_v[j] = mixed

    def put_result(j, top, total, mixed):
        att[:, j * head_dim : (j + 1) * head_dim] = (mixed / total).astype(jnp.bfloat16)

    def other(owner, i):
        q = nearest(owner, patches, i)
        return stale_all.at[q], lens[q]

    every = list(range(heads))
    kept = list(range(SHIP, heads))
    shipped = list(range(SHIP))
    is_end = first_end | last_end
    is_host = to_first | to_last
    lane = lax.broadcasted_iota(jnp.int32, (patch_tok, head_dim), 1)
    home = to_last.astype(jnp.int32) * (patches - 1)

    def back_copies(to):
        return (
            remote(guest_o, home_o, go_s, go_r, {"patch": to}),
            remote(guest_n, home_n, gn_s, gn_r, {"patch": to}),
        )

    def put_guest(j, top, total, mixed):
        guest_o[j] = (mixed / total).astype(jnp.bfloat16)
        notes = jnp.where(lane == 0, top, jnp.where(lane == 1, total, 0.0))
        guest_n[j] = jnp.transpose(notes, (1, 0))[0:8]

    attend_part([(ncbuf, lens[p])], every, qbuf, True, keep_part)
    relay_to(len(relays) - 1)

    @pl.when(is_host)
    def _():
        guest_copy(0).wait_recv()
        sources = [other(home, i) for i in range(patches - 1)]
        attend_part(sources, shipped, guest_q, True, put_guest)
        for back in back_copies(home):
            back.start()

    relay_to(len(relays))

    @pl.when(p * (patches - 1 - p) > 0)
    def _():
        sources = [other(p, i) for i in range(patches - 1)]
        attend_part(sources, every, qbuf, False, put_result)

    @pl.when(is_end)
    def _():
        end_arrivals(range(1, patches - 1))
        sources = [other(p, i) for i in range(patches - 2)]
        attend_part(sources, kept, qbuf, False, keep_part)

    end_arrivals([patches - 1])

    @pl.when(is_end)
    def _():
        attend_part([other(p, patches - 2)], kept, qbuf, False, put_result)


    @pl.when(is_end)
    def _():
        for back in back_copies(home):
            back.wait_recv()
        for j in shipped:
            notes = jnp.concatenate(
                [home_n[j], jnp.zeros((patch_tok - 8, patch_tok), jnp.float32)], axis=0
            )
            notes = jnp.transpose(notes, (1, 0))
            top, total = notes[:, 0:1], notes[:, 1:2]
            highest = jnp.maximum(top, top_v[j])
            away = total * jnp.exp(top - highest)
            here = jnp.exp(top_v[j] - highest)
            mixed = home_o[j].astype(jnp.float32) * away + out_v[j] * here
            put_result(j, highest, away + den_v[j] * here, mixed)

    ow_copy.wait()

    cuts = []
    for units in OUT_SPLIT:
        begin = cuts[-1].stop if cuts else 0
        cuts.append(slice(begin, begin + units * (width // sum(OUT_SPLIT))))
    ranges = [pl.ds(cut.start, cut.stop - cut.start) for cut in cuts]

    def near_copy(c):
        cols = ranges[c]
        return remote(pbuf.at[slot[1], :, cols], dbuf.at[0, :, cols], d_s, d_r, dev[1])

    def pair_copy(c):
        cols = ranges[c]
        return remote(pbuf.at[slot[3], :, cols], dbuf.at[1, :, cols], e_s, e_r.at[c - 1], dev[1])

    def raw_copy(k):
        cols = ranges[0]
        return remote(pbuf.at[slot[k], :, cols], raw.at[k - 2], raw_s, raw_r, dev[k])

    def x_copy(c):
        cols = ranges[c]
        return remote(xs.at[:, cols], xr.at[:, cols], x_s, x_r.at[c - 1], dev[2])

    rows_att = att[...]
    flat = heads * head_dim
    for c, cut in enumerate(cuts):
        piece = jnp.dot(
            rows_att,
            ow_v[:, :, cut].reshape(flat, cut.stop - cut.start),
            preferred_element_type=jnp.float32,
        )
        pbuf[:, :, cut] = piece.astype(jnp.bfloat16).reshape(group, rows, cut.stop - cut.start)
        if c == 0:
            raw_copy(2).start()
            raw_copy(3).start()
        else:
            pair_copy(c).start()
        near_copy(c).start()
    for c in range(1, len(cuts)):
        pair_copy(c).wait_recv()
        cut = cuts[c]
        xs[:, cut] = (
            pbuf[slot[2], :, cut].astype(jnp.float32) + dbuf[1, :, cut].astype(jnp.float32)
        ).astype(jnp.bfloat16)
        x_copy(c).start()

    ncrecv[slot[0]] = ncbuf[slot[0]]
    three = ncrecv.at[pl.ds(0, group - 1)]
    remote(three, three, nc_s, nc_r, dev[1]).wait_recv()
    landed = ncrecv[...].reshape(group * heads, rows, 2 * head_dim)
    nc_out[...] = jnp.transpose(landed, (1, 0, 2))

    sent = st_t.at[pl.ds(0, (group - 1) * heads)]
    remote(sent, sent, st_send, st_recv.at[0], dev[1]).wait_send()
    remote(three, three, nc_s, nc_r, dev[1]).wait_send()
    for sem in (na_s, nb_s, nr_s):
        remote(beside, beside, sem, na_r, dev[1]).wait_send()
    for q in range(patches):
        whole = stale_all.at[q]
        outer = stale_all.at[q, :, pl.ds(SHIP, heads - SHIP)]

        @pl.when((p < patches - 2) & (q <= p))
        def _():
            remote(whole, whole, zs_r.at[q], z_recv.at[q, 0], {"patch": p + 1}).wait_send()

        @pl.when(to_last & (q <= p) & (q + 2 > p))
        def _():
            remote(outer, outer, zs_r.at[q], z_recv.at[q, 0], {"patch": p + 1}).wait_send()

        @pl.when((p > 1) & (q >= p))
        def _():
            remote(whole, whole, zs_l.at[q], z_recv.at[q, 0], {"patch": p - 1}).wait_send()

        @pl.when(to_first & (q >= p) & (q < p + 2))
        def _():
            remote(outer, outer, zs_l.at[q], z_recv.at[q, 0], {"patch": p - 1}).wait_send()

    @pl.when(is_end)
    def _():
        guest_copy(0).wait_send()

    far_part = stale_all.at[0, pl.ds(0, group - 1), pl.ds(SHIP, heads - SHIP)]

    @pl.when(to_last)
    def _():
        remote(far_part, far_part, zs_r.at[0], z_recv.at[0, 0], {"patch": p + 1}).wait_send()
        z_straight(False).wait_send()

    @pl.when(to_first)
    def _():
        last_q = patches - 1
        remote(
            far_part, far_part, zs_l.at[last_q], z_recv.at[0, 0], {"patch": p - 1}
        ).wait_send()
        z_straight(True).wait_send()

    @pl.when(is_host)
    def _():
        for back in back_copies(home):
            back.wait_send()

    near = dbuf.at[0]
    remote(near, near, d_s, d_r, dev[1]).wait_recv()
    remote(raw, raw, raw_s, raw_r, dev[2]).wait_recv()
    for c, cut in enumerate(cuts):
        total = pbuf[slot[0], :, cut].astype(jnp.float32) + dbuf[0, :, cut].astype(jnp.float32)
        if c == 0:
            total = total + raw[0].astype(jnp.float32) + raw[1].astype(jnp.float32)
        else:
            x_copy(c).wait_recv()
            total = total + xr[:, cut].astype(jnp.float32)
        upd[:, cut] = (mod[2:3, cut] * total).astype(jnp.bfloat16)
    remote(near, near, d_s, d_r, dev[1]).wait_send()
    remote(raw, raw, raw_s, raw_r, dev[2]).wait_send()
    rest = pl.ds(cuts[1].start, width - cuts[1].start)
    remote(dbuf.at[1, :, rest], dbuf.at[1, :, rest], e_s, e_r.at[0], dev[1]).wait_send()
    remote(xs.at[:, rest], xs.at[:, rest], x_s, x_r.at[0], dev[2]).wait_send()


def store_kernel(upd, cache, upd_out, cache_out, sems):
    first = pltpu.make_async_copy(upd, upd_out, sems.at[0])
    second = pltpu.make_async_copy(cache, cache_out, sems.at[1])
    first.start()
    second.start()
    first.wait()
    second.wait()


def fused_device(
    patches, tokens, modulation, in_weight, query_gain, key_gain, out_weight, stale_cache, lengths
):
    rows, width = tokens.shape
    heads, head_dim = out_weight.shape[:2]
    group = 4
    all_heads = stale_cache.shape[1]
    patch_tok = rows * group
    bf, f32 = jnp.bfloat16, jnp.float32
    raw_cols = OUT_SPLIT[0] * (width // sum(OUT_SPLIT))
    later = len(OUT_SPLIT) - 1
    vm = pl.BlockSpec(memory_space=pltpu.VMEM)
    dma = pltpu.SemaphoreType.DMA
    upd, cache = pl.pallas_call(
        functools.partial(fused_kernel, patches=patches),
        out_shape=(
            jax.ShapeDtypeStruct((rows, width), bf),
            jax.ShapeDtypeStruct((rows, all_heads, 2 * head_dim), bf),
        ),
        in_specs=[pl.BlockSpec(memory_space=pltpu.HBM)] * 8,
        out_specs=(vm, vm),
        scratch_shapes=[
            pltpu.VMEM(tokens.shape, bf),
            pltpu.VMEM(modulation.shape, f32),
            pltpu.VMEM((1, head_dim), f32),
            pltpu.VMEM((1, head_dim), f32),
            pltpu.SMEM(lengths.shape, jnp.int32),
            pltpu.VMEM(stale_cache.shape, bf),
            pltpu.VMEM(in_weight.shape, bf),
            pltpu.VMEM((width, heads * 3 * head_dim), bf),
            pltpu.VMEM(out_weight.shape, bf),
            pltpu.VMEM((all_heads, rows, 2 * head_dim), bf),
            pltpu.VMEM((group, rows, width), bf),
            pltpu.VMEM((patch_tok, heads * 3 * head_dim), f32),
            pltpu.VMEM((patches, group, heads, rows, 2 * head_dim), bf),
            pltpu.VMEM((group, heads, rows, 2 * head_dim), bf),
            pltpu.VMEM((group, heads, rows, 2 * head_dim), bf),
            pltpu.VMEM((heads, patch_tok, head_dim), bf),
            pltpu.VMEM((heads, patch_tok, 1), f32),
            pltpu.VMEM((heads, patch_tok, 1), f32),
            pltpu.VMEM((heads, patch_tok, head_dim), f32),
            pltpu.VMEM((patch_tok, heads * head_dim), bf),
            pltpu.VMEM((group, rows, width), bf),
            pltpu.VMEM((2, rows, width), bf),
            pltpu.VMEM((2, rows, raw_cols), bf),
            pltpu.VMEM((rows, width), bf),
            pltpu.VMEM((rows, width), bf),
            pltpu.VMEM((SHIP, patch_tok, head_dim), bf),
            pltpu.VMEM((SHIP, patch_tok, head_dim), bf),
            pltpu.VMEM((SHIP, 8, patch_tok), f32),
            pltpu.VMEM((SHIP, patch_tok, head_dim), bf),
            pltpu.VMEM((SHIP, 8, patch_tok), f32),
            dma((6,)), dma((K_CHUNKS,)), dma, dma, dma((3,)),
            dma((patches,)), dma((patches,)), dma((patches - 1, 5)),
            dma, dma, dma, dma, dma((K_CHUNKS,)), dma((K_CHUNKS,)), dma, dma,
            dma, dma, dma, dma((later,)), dma, dma, dma, dma((later,)),
            dma, dma, dma, dma, dma, dma, dma,
        ],
        compiler_params=pltpu.CompilerParams(
            collective_id=0, has_side_effects=True, vmem_limit_bytes=48 * 1024 * 1024
        ),
    )(
        *[
            pltpu.with_memory_space_constraint(operand, pltpu.HBM)
            for operand in (
                tokens, modulation, query_gain.reshape(1, -1), key_gain.reshape(1, -1), lengths,
                stale_cache, in_weight, out_weight,
            )
        ]
    )
    return pl.pallas_call(
        store_kernel,
        out_shape=(
            jax.ShapeDtypeStruct(upd.shape, upd.dtype),
            jax.ShapeDtypeStruct(cache.shape, cache.dtype),
        ),
        in_specs=[vm, vm],
        out_specs=[pl.BlockSpec(memory_space=pltpu.HBM)] * 2,
        scratch_shapes=[dma((2,))],
        compiler_params=pltpu.CompilerParams(vmem_limit_bytes=4 * 1024 * 1024),
    )(upd, cache)


def choose(
    patches, group_shape, tokens, modulation, in_weight, query_gain, key_gain, out_weight,
    stale_cache, lengths,
):
    rows, width = tokens.shape
    heads, head_dim = out_weight.shape[:2]
    kv_bytes = patches * 4 * heads * rows * 4 * head_dim
    weight_bytes = 2 * (in_weight.size + out_weight.size)
    fits = (
        group_shape == (2, 2)
        and rows % 16 == 0
        and head_dim % 128 == 0
        and width % (128 * K_CHUNKS) == 0
        and width % (128 * sum(OUT_SPLIT)) == 0
        and width % (TURN * K_CHUNKS) == 0
        and patches == 4
        and heads > SHIP
        and rows * 4 == head_dim
        and rows * 4 * patches <= 1024
        and kv_bytes + weight_bytes <= 24 * 1024 * 1024
    )
    args = (
        tokens, modulation, in_weight, query_gain, key_gain, out_weight, stale_cache, lengths
    )
    return fused_device(patches, *args) if fits else per_device(*args)


def solution(mesh):
    return jax.shard_map(
        functools.partial(
            choose, mesh.shape["patch"], (mesh.shape["head"], mesh.shape["rep"])
        ),
        mesh=mesh,
        in_specs=(
            P(("clip", "patch", "head", "rep"), None),
            P(),
            P(None, ("head", "rep"), None),
            P(),
            P(),
            P(("head", "rep"), None, None),
            P(("clip", "patch", "head", "rep"), None, None),
            P("clip"),
        ),
        out_specs=(
            P(("clip", "patch", "head", "rep"), None),
            P(("clip", "patch", "head", "rep"), None, None),
        ),
        check_vma=False,
    )
```

```python
import functools
import math

import jax
import jax.numpy as jnp
from jax import lax
from jax.experimental import pallas as pl
from jax.experimental.pallas import tpu as pltpu
from jax.sharding import PartitionSpec as P

EPSILON = 1e-06
NEGATIVE = -1e30
key_block = 512


def normalize_rows(values):
    average = jnp.mean(values, axis=-1, keepdims=True)
    centred = values - average
    variance = jnp.mean(centred * centred, axis=-1, keepdims=True)
    return centred * lax.rsqrt(variance + EPSILON)


def rms_gain(values, gain):
    return values * lax.rsqrt(jnp.mean(values * values, axis=-1, keepdims=True) + EPSILON) * gain


def project(normed, in_weight, query_gain, key_gain):
    row_count = normed.shape[0]
    head_count = in_weight.shape[1]
    triple = in_weight.shape[2]
    head_dim = triple // 3
    flat_weight = in_weight.reshape(in_weight.shape[0], head_count * triple)
    projected = jnp.dot(normed, flat_weight, preferred_element_type=jnp.float32).reshape(
        row_count, head_count, triple
    )
    queries = rms_gain(projected[..., :head_dim], query_gain)
    fresh_keys = rms_gain(projected[..., head_dim : 2 * head_dim], key_gain)
    return jnp.concatenate([queries, fresh_keys, projected[..., 2 * head_dim :]], axis=-1).astype(
        jnp.bfloat16
    )


def lookup(lengths, patch_of):
    patch_ids = jnp.arange(lengths.shape[0], dtype=jnp.int32)
    return jnp.sum(jnp.where(patch_of[:, None] == patch_ids[None, :], lengths[None, :], 0), axis=1)


def attend(running, queries, key_rows, usable):
    head_dim = queries.shape[-1]
    row_max, denominator, weighted = running
    scores = jnp.einsum(
        "qhd,khd->qhk", queries, key_rows[..., :head_dim], preferred_element_type=jnp.float32
    )
    scores = scores * (1.0 / math.sqrt(head_dim))
    key_mask = usable[None, None, :]
    scores = jnp.where(key_mask, scores, NEGATIVE)
    new_max = jnp.maximum(row_max, jnp.max(scores, axis=-1))
    weights = jnp.where(key_mask, jnp.exp(scores - new_max[..., None]), 0.0)
    factor = jnp.exp(row_max - new_max)
    denominator = denominator * factor + jnp.sum(weights, axis=-1)
    weighted = weighted * factor[..., None] + jnp.einsum(
        "qhk,khd->qhd",
        weights.astype(jnp.bfloat16),
        key_rows[..., head_dim:],
        preferred_element_type=jnp.float32,
    )
    return (new_max, denominator, weighted)


def attend_blocks(running, queries, key_rows, usable):
    key_count = key_rows.shape[0]
    if key_count > key_block and key_count % key_block == 0:
        shaped = key_rows.reshape((key_count // key_block, key_block) + key_rows.shape[1:])
        usable_rows = usable.reshape(key_count // key_block, key_block)

        def step_block(current, operands):
            return (attend(current, queries, operands[0], operands[1]), None)

        running, _ = lax.scan(step_block, running, (shaped, usable_rows))
        return running
    return attend(running, queries, key_rows, usable)


def per_device(
    tokens, modulation, in_weight, query_gain, key_gain, out_weight, stale_cache, lengths
):
    heads_dev = in_weight.shape[1]
    head_dim = query_gain.shape[0]
    normed = (
        normalize_rows(tokens.astype(jnp.float32)) * (1.0 + modulation[1]) + modulation[0]
    ).astype(jnp.bfloat16)
    fresh = project(
        lax.all_gather(normed, ("head", "rep"), axis=0, tiled=True), in_weight, query_gain, key_gain
    )
    queries = fresh[..., :head_dim]
    own_rows = fresh[..., head_dim:]
    new_cache = lax.all_to_all(own_rows, ("head", "rep"), split_axis=0, concat_axis=1, tiled=True)
    patch_tok = fresh.shape[0]
    own_patch = lax.axis_index("patch")
    own_length = lookup(lengths, jnp.full((1,), own_patch, jnp.int32))[0]
    running = (
        jnp.full((patch_tok, heads_dev), NEGATIVE, jnp.float32),
        jnp.zeros((patch_tok, heads_dev), jnp.float32),
        jnp.zeros((patch_tok, heads_dev, head_dim), jnp.float32),
    )
    running = attend_blocks(
        running, queries, own_rows, jnp.arange(patch_tok, dtype=jnp.int32) < own_length
    )
    stale_heads = lax.all_to_all(
        stale_cache, ("head", "rep"), split_axis=1, concat_axis=0, tiled=True
    )
    shard_part = lax.all_gather(stale_heads, "patch", axis=0, tiled=True)
    key_index = jnp.arange(shard_part.shape[0], dtype=jnp.int32)
    patch_of = key_index // patch_tok
    position = key_index % patch_tok
    usable = (position < lookup(lengths, patch_of)) & (patch_of != own_patch)
    running = attend_blocks(running, queries, shard_part, usable)
    attended = (running[2] / running[1][..., None]).astype(jnp.bfloat16)
    flat_rows = attended.reshape(patch_tok, heads_dev * head_dim)
    flat_weight = out_weight.reshape(heads_dev * head_dim, out_weight.shape[2])
    attention = lax.psum_scatter(
        jnp.dot(flat_rows, flat_weight, preferred_element_type=jnp.float32).astype(jnp.bfloat16),
        ("head", "rep"),
        scatter_dimension=0,
        tiled=True,
    ).astype(jnp.float32)
    update = (modulation[2] * attention).astype(jnp.bfloat16)
    return (update, new_cache)


MESH = pl.DeviceIdType.MESH
K_CHUNKS = 4
OUT_SPLIT = (4, 8, 12)
TURN = 64
SHIP = 1
RELAY_ORDER = ((1, 0), (1, 1), (1, 2), (2, 0), (2, 1), (1, 3), (1, 4), (2, 2), (2, 3), (2, 4))
RELAYS = (1, 2, 4, 5, 7, 7, 8)


def nearest(p, patches, i):
    place = 0
    for own in range(patches):
        others = sorted((q for q in range(patches) if q != own), key=lambda q: (abs(q - own), q))
        place = place + (p == own).astype(jnp.int32) * others[i]
    return place


def fused_kernel(
    tok_hbm, mod_hbm, qg_hbm, kg_hbm, lens_hbm, st_hbm, w_hbm, ow_hbm, upd, nc_out,
    tok, mod, qg, kg, lens, st,
    w_raw, w_v, ow_v, st_t, normed_all, acc, stale_all, ncbuf, ncrecv,
    qbuf, top_v, den_v, out_v, att, pbuf, dbuf, raw, xs, xr,
    guest_q, guest_o, guest_n, home_o, home_n,
    in_sem, w_sem, ow_sem, st_send, st_recv, zs_r, zs_l, z_recv,
    na_s, nb_s, nr_s, na_r, nb_r, nr_r, nc_s, nc_r,
    d_s, d_r, e_s, e_r, raw_s, raw_r, x_s, x_r, far_s, gq_s, gq_r, go_s, go_r, gn_s, gn_r,
    *, patches,
):
    p = lax.axis_index("patch")
    h = lax.axis_index("head")
    r = lax.axis_index("rep")
    heads = ow_hbm.shape[0]
    head_dim = ow_hbm.shape[1]
    rows, width = tok.shape
    triple = 3 * head_dim
    kc = width // K_CHUNKS
    group = 4
    patch_tok = group * rows
    coords = [(h, r), (h, 1 - r), (1 - h, r), (1 - h, 1 - r)]
    slot = [a * 2 + b for a, b in coords]
    dev = [{"head": a, "rep": b} for a, b in coords]

    def remote(src, dst, ss, rs, to):
        return pltpu.make_async_remote_copy(
            src_ref=src, dst_ref=dst, send_sem=ss, recv_sem=rs, device_id=to, device_id_type=MESH
        )

    loads = [
        pltpu.make_async_copy(src, dst, in_sem.at[i])
        for i, (src, dst) in enumerate(
            [(st_hbm, st), (tok_hbm, tok), (mod_hbm, mod), (qg_hbm, qg), (kg_hbm, kg), (lens_hbm, lens)]
        )
    ]
    for load in loads:
        load.start()

    has_right = p + 1 < patches
    has_left = p > 0
    barrier = pltpu.get_barrier_semaphore()
    for k in (1, 2, 3):
        pl.semaphore_signal(barrier, inc=1, device_id=dev[k], device_id_type=MESH)

    @pl.when(has_right)
    def _():
        pl.semaphore_signal(barrier, inc=1, device_id={"patch": p + 1}, device_id_type=MESH)

    @pl.when(has_left)
    def _():
        pl.semaphore_signal(barrier, inc=1, device_id={"patch": p - 1}, device_id_type=MESH)

    def w_copy(c):
        return pltpu.make_async_copy(
            w_hbm.at[pl.ds(c * kc, kc)], w_raw.at[pl.ds(c * kc, kc)], w_sem.at[c]
        )

    def w_turn(c):
        w_copy(c).wait()

        @pl.loop(0, kc // TURN)
        def _(i):
            at = pl.multiple_of(c * kc + i * TURN, TURN)
            turned = jnp.transpose(w_raw[pl.ds(at, TURN)], (1, 0, 2))
            for j in range(heads):
                w_v[pl.ds(at, TURN), j * triple : (j + 1) * triple] = turned[j]

    for c in range(K_CHUNKS):
        w_copy(c).start()
    ow_copy = pltpu.make_async_copy(ow_hbm, ow_v, ow_sem)
    ow_copy.start()

    loads[0].wait()
    st_t[...] = jnp.transpose(st[...], (1, 0, 2))
    stale_all[p, slot[0], 0:SHIP] = st_t[pl.ds(slot[0] * heads, SHIP)]

    pl.semaphore_wait(barrier, 3 + has_right.astype(jnp.int32) + has_left.astype(jnp.int32))

    def stale_part(k):
        return st_t.at[pl.ds(slot[k] * heads, heads)]

    def stale_copy(k):
        return remote(
            stale_part(k), stale_all.at[p, slot[0]], st_send, st_recv.at[k - 1], dev[k]
        )

    def stale_arrival(k):
        place = stale_all.at[p, slot[k]]
        remote(place, place, st_send, st_recv.at[k - 1], dev[k]).wait_recv()

    first_end, last_end = p == 0, p == patches - 1
    to_last, to_first = p == patches - 2, p == 1

    def landing(q, step, k):
        return z_recv.at[(q - p - step + patches) % patches - 1, k]

    def z_copy(q, k, right, outer, own=False):
        begin = SHIP if outer or k == 4 else 0
        end = SHIP if k == 3 else heads
        place = stale_all.at[q, slot[min(k, 3)], pl.ds(begin, end - begin)]
        src = place
        if own and k == 0:
            src = st_t.at[pl.ds(slot[0] * heads + begin, end - begin)]
        if right:
            return remote(src, place, zs_r.at[q], landing(q, 1, k), {"patch": p + 1})
        return remote(src, place, zs_l.at[q], landing(q, -1, k), {"patch": p - 1})

    def z_landed(q, k, outer):
        begin = SHIP if outer or k == 4 else 0
        end = SHIP if k == 3 else heads
        place = stale_all.at[q, slot[min(k, 3)], pl.ds(begin, end - begin)]
        remote(place, place, far_s, landing(q, 0, k), dev[1]).wait_recv()

    def z_send(q, k, right, own=False):
        if k != 3:

            @pl.when(to_last if right else to_first)
            def _():
                z_copy(q, k, right, True, own).start()

        @pl.when((p < patches - 2) if right else (p > 1))
        def _():
            z_copy(q, k, right, False, own).start()

    def z_own(k):
        z_send(p, k, True, k == 0)
        z_send(p, k, False, k == 0)

    def z_straight(right):
        q = 0 if right else patches - 1
        place = stale_all.at[q, slot[3], pl.ds(SHIP, heads - SHIP)]
        step = 2 if right else -2
        return remote(place, place, far_s, landing(q, step, 4), {"patch": p + step})

    def z_relay(d, k):
        @pl.when((p - d >= 0) & (p < patches - 1))
        def _():
            z_landed(p - d, k, False)
            if (d, k) != (2, 4):
                z_send(p - d, k, True)

        @pl.when((p + d < patches) & (p > 0))
        def _():
            z_landed(p + d, k, False)
            if (d, k) != (2, 4):
                z_send(p + d, k, False)

        if (d, k) == (1, 4):

            @pl.when(to_first)
            def _():
                z_straight(True).start()

            @pl.when(to_last)
            def _():
                z_straight(False).start()

    def end_arrivals(distances):
        for d in distances:
            for k in (0, 1, 2, 4):

                @pl.when((p - d >= 0) & last_end)
                def _():
                    z_landed(p - d, k, True)

                @pl.when((p + d < patches) & first_end)
                def _():
                    z_landed(p + d, k, True)

    def chunk(k, c):
        return normed_all.at[slot[k], :, pl.ds(c * kc, kc)]

    def feature_across(c):
        return remote(chunk(0, c), chunk(0, c), nb_s, nb_r.at[c], dev[2])

    def feature_beside():
        place = normed_all.at[slot[0]]
        return remote(place, place, na_s, na_r, dev[1])

    def feature_relay(c):
        return remote(chunk(2, c), chunk(2, c), nr_s, nr_r.at[c], dev[1])

    def feature_pass(c):
        remote(chunk(2, c), chunk(2, c), nb_s, nb_r.at[c], dev[2]).wait_recv()
        feature_relay(c).start()

    relays = RELAY_ORDER
    done = [0]

    def relay_to(count):
        for d, k in relays[done[0] : count]:
            z_relay(d, k)
        done[0] = max(done[0], count)

    z_own(0)
    for k in (2, 3, 1):
        stale_copy(k).start()
    loads[1].wait()
    loads[2].wait()
    values = tok[...].astype(jnp.float32)
    normed = (normalize_rows(values) * (1.0 + mod[1:2, :]) + mod[0:1, :]).astype(jnp.bfloat16)
    normed_all[slot[0]] = normed
    for c in range(K_CHUNKS):
        feature_across(c).start()
    feature_beside().start()
    stale_arrival(1)
    z_own(1)
    w_turn(0)
    w_turn(1)
    relay_to(RELAYS[0])
    stale_arrival(2)
    z_own(2)
    w_turn(2)
    relay_to(RELAYS[1])
    stale_arrival(3)
    z_own(3)
    z_own(4)
    for c in range(3, K_CHUNKS):
        w_turn(c)
    feature_pass(0)
    beside = normed_all.at[slot[1]]
    remote(beside, beside, na_s, na_r, dev[1]).wait_recv()
    for c in range(K_CHUNKS):
        if c + 1 < K_CHUNKS:
            feature_pass(c + 1)
        remote(chunk(3, c), chunk(3, c), nr_s, nr_r.at[c], dev[1]).wait_recv()
        part = normed_all[:, :, c * kc : (c + 1) * kc].reshape(patch_tok, kc)
        product = jnp.dot(
            part, w_v[c * kc : (c + 1) * kc, :], preferred_element_type=jnp.float32
        )
        if c == 0:
            acc[...] = product
        else:
            acc[...] += product
        relay_to(RELAYS[2 + c])

    for load in loads[3:]:
        load.wait()
    q_gain = qg[...]
    k_gain = kg[...]
    def query_of(j):
        base = j * triple
        qbuf[j] = rms_gain(acc[:, base : base + head_dim], q_gain).astype(jnp.bfloat16)

    for j in range(SHIP):
        query_of(j)
    leaving = qbuf.at[pl.ds(0, SHIP)]

    def guest_copy(step):
        return remote(leaving, guest_q, gq_s, gq_r, {"patch": p + step})

    @pl.when(first_end)
    def _():
        guest_copy(1).start()

    @pl.when(last_end)
    def _():
        guest_copy(-1).start()

    for j in range(heads):
        base = j * triple
        keys = rms_gain(acc[:, base + head_dim : base + 2 * head_dim], k_gain).astype(jnp.bfloat16)
        ncbuf[:, j, :, :head_dim] = keys.reshape(group, rows, head_dim)
        ncbuf[:, j, :, head_dim:] = (
            acc[:, base + 2 * head_dim : base + triple]
            .astype(jnp.bfloat16)
            .reshape(group, rows, head_dim)
        )
        if j >= SHIP:
            query_of(j)

    def cache_copy(k):
        return remote(
            ncbuf.at[slot[k]], ncrecv.at[slot[0]], nc_s, nc_r, dev[k]
        )

    for k in (2, 3, 1):
        cache_copy(k).start()
    relay_to(RELAYS[2 + K_CHUNKS])
    scale = 1.0 / math.sqrt(head_dim)
    columns = lax.broadcasted_iota(jnp.int32, (1, patch_tok), 1)
    contract = (((1,), (1,)), ((), ()))

    def attend_part(sources, used, asking, first, finish):
        masks = [columns < live for _, live in sources]
        scores = {
            j: [
                lax.dot_general(
                    asking[j],
                    source[:, j, :, :head_dim].reshape(patch_tok, head_dim),
                    contract,
                    preferred_element_type=jnp.float32,
                )
                for source, _ in sources
            ]
            for j in used
        }
        scores = {
            j: [jnp.where(mask, part * scale, NEGATIVE) for part, mask in zip(scores[j], masks)]
            for j in used
        }
        tops = {
            j: functools.reduce(
                jnp.maximum, [jnp.max(part, axis=1, keepdims=True) for part in scores[j]]
            )
            for j in used
        }
        if not first:
            before = {j: top_v[j] for j in used}
            tops = {j: jnp.maximum(before[j], tops[j]) for j in used}
            factor = {j: jnp.exp(before[j] - tops[j]) for j in used}
        weights = {
            j: [
                jnp.where(mask, jnp.exp(part - tops[j]), 0.0)
                for part, mask in zip(scores[j], masks)
            ]
            for j in used
        }
        mixed = {
            j: sum(
                jnp.dot(
                    part.astype(jnp.bfloat16),
                    source[:, j, :, head_dim:].reshape(patch_tok, head_dim),
                    preferred_element_type=jnp.float32,
                )
                for part, (source, _) in zip(weights[j], sources)
            )
            for j in used
        }
        total = {
            j: sum(jnp.sum(part, axis=1, keepdims=True) for part in weights[j]) for j in used
        }
        if not first:
            total = {j: total[j] + den_v[j] * factor[j] for j in used}
            mixed = {j: mixed[j] + out_v[j] * factor[j] for j in used}
        for j in used:
            finish(j, tops[j], total[j], mixed[j])

    def keep_part(j, top, total, mixed):
        top_v[j] = top
        den_v[j] = total
        out_v[j] = mixed

    def put_result(j, top, total, mixed):
        att[:, j * head_dim : (j + 1) * head_dim] = (mixed / total).astype(jnp.bfloat16)

    def other(owner, i):
        q = nearest(owner, patches, i)
        return stale_all.at[q], lens[q]

    every = list(range(heads))
    kept = list(range(SHIP, heads))
    shipped = list(range(SHIP))
    is_end = first_end | last_end
    is_host = to_first | to_last
    lane = lax.broadcasted_iota(jnp.int32, (patch_tok, head_dim), 1)
    home = to_last.astype(jnp.int32) * (patches - 1)

    def back_copies(to):
        return (
            remote(guest_o, home_o, go_s, go_r, {"patch": to}),
            remote(guest_n, home_n, gn_s, gn_r, {"patch": to}),
        )

    def put_guest(j, top, total, mixed):
        guest_o[j] = (mixed / total).astype(jnp.bfloat16)
        notes = jnp.where(lane == 0, top, jnp.where(lane == 1, total, 0.0))
        guest_n[j] = jnp.transpose(notes, (1, 0))[0:8]

    attend_part([(ncbuf, lens[p])], every, qbuf, True, keep_part)
    relay_to(len(relays) - 1)

    @pl.when(is_host)
    def _():
        guest_copy(0).wait_recv()
        sources = [other(home, i) for i in range(patches - 1)]
        attend_part(sources, shipped, guest_q, True, put_guest)
        for back in back_copies(home):
            back.start()

    relay_to(len(relays))

    @pl.when(p * (patches - 1 - p) > 0)
    def _():
        sources = [other(p, i) for i in range(patches - 1)]
        attend_part(sources, every, qbuf, False, put_result)

    @pl.when(is_end)
    def _():
        end_arrivals(range(1, patches - 1))
        sources = [other(p, i) for i in range(patches - 2)]
        attend_part(sources, kept, qbuf, False, keep_part)

    end_arrivals([patches - 1])

    @pl.when(is_end)
    def _():
        attend_part([other(p, patches - 2)], kept, qbuf, False, put_result)


    @pl.when(is_end)
    def _():
        for back in back_copies(home):
            back.wait_recv()
        for j in shipped:
            notes = jnp.concatenate(
                [home_n[j], jnp.zeros((patch_tok - 8, patch_tok), jnp.float32)], axis=0
            )
            notes = jnp.transpose(notes, (1, 0))
            top, total = notes[:, 0:1], notes[:, 1:2]
            highest = jnp.maximum(top, top_v[j])
            away = total * jnp.exp(top - highest)
            here = jnp.exp(top_v[j] - highest)
            mixed = home_o[j].astype(jnp.float32) * away + out_v[j] * here
            put_result(j, highest, away + den_v[j] * here, mixed)

    ow_copy.wait()

    cuts = []
    for units in OUT_SPLIT:
        begin = cuts[-1].stop if cuts else 0
        cuts.append(slice(begin, begin + units * (width // sum(OUT_SPLIT))))
    ranges = [pl.ds(cut.start, cut.stop - cut.start) for cut in cuts]

    def near_copy(c):
        cols = ranges[c]
        return remote(pbuf.at[slot[1], :, cols], dbuf.at[0, :, cols], d_s, d_r, dev[1])

    def pair_copy(c):
        cols = ranges[c]
        return remote(pbuf.at[slot[3], :, cols], dbuf.at[1, :, cols], e_s, e_r.at[c - 1], dev[1])

    def raw_copy(k):
        cols = ranges[0]
        return remote(pbuf.at[slot[k], :, cols], raw.at[k - 2], raw_s, raw_r, dev[k])

    def x_copy(c):
        cols = ranges[c]
        return remote(xs.at[:, cols], xr.at[:, cols], x_s, x_r.at[c - 1], dev[2])

    rows_att = att[...]
    flat = heads * head_dim
    for c, cut in enumerate(cuts):
        piece = jnp.dot(
            rows_att,
            ow_v[:, :, cut].reshape(flat, cut.stop - cut.start),
            preferred_element_type=jnp.float32,
        )
        pbuf[:, :, cut] = piece.astype(jnp.bfloat16).reshape(group, rows, cut.stop - cut.start)
        if c == 0:
            raw_copy(2).start()
            raw_copy(3).start()
        else:
            pair_copy(c).start()
        near_copy(c).start()
    for c in range(1, len(cuts)):
        pair_copy(c).wait_recv()
        cut = cuts[c]
        xs[:, cut] = (
            pbuf[slot[2], :, cut].astype(jnp.float32) + dbuf[1, :, cut].astype(jnp.float32)
        ).astype(jnp.bfloat16)
        x_copy(c).start()

    ncrecv[slot[0]] = ncbuf[slot[0]]
    three = ncrecv.at[pl.ds(0, group - 1)]
    remote(three, three, nc_s, nc_r, dev[1]).wait_recv()
    landed = ncrecv[...].reshape(group * heads, rows, 2 * head_dim)
    nc_out[...] = jnp.transpose(landed, (1, 0, 2))

    sent = st_t.at[pl.ds(0, (group - 1) * heads)]
    remote(sent, sent, st_send, st_recv.at[0], dev[1]).wait_send()
    remote(three, three, nc_s, nc_r, dev[1]).wait_send()
    for sem in (na_s, nb_s, nr_s):
        remote(beside, beside, sem, na_r, dev[1]).wait_send()
    for q in range(patches):
        whole = stale_all.at[q]
        outer = stale_all.at[q, :, pl.ds(SHIP, heads - SHIP)]

        @pl.when((p < patches - 2) & (q <= p))
        def _():
            remote(whole, whole, zs_r.at[q], z_recv.at[q, 0], {"patch": p + 1}).wait_send()

        @pl.when(to_last & (q <= p) & (q + 2 > p))
        def _():
            remote(outer, outer, zs_r.at[q], z_recv.at[q, 0], {"patch": p + 1}).wait_send()

        @pl.when((p > 1) & (q >= p))
        def _():
            remote(whole, whole, zs_l.at[q], z_recv.at[q, 0], {"patch": p - 1}).wait_send()

        @pl.when(to_first & (q >= p) & (q < p + 2))
        def _():
            remote(outer, outer, zs_l.at[q], z_recv.at[q, 0], {"patch": p - 1}).wait_send()

    @pl.when(is_end)
    def _():
        guest_copy(0).wait_send()

    far_part = stale_all.at[0, pl.ds(0, group - 1), pl.ds(SHIP, heads - SHIP)]

    @pl.when(to_last)
    def _():
        remote(far_part, far_part, zs_r.at[0], z_recv.at[0, 0], {"patch": p + 1}).wait_send()
        z_straight(False).wait_send()

    @pl.when(to_first)
    def _():
        last_q = patches - 1
        remote(
            far_part, far_part, zs_l.at[last_q], z_recv.at[0, 0], {"patch": p - 1}
        ).wait_send()
        z_straight(True).wait_send()

    @pl.when(is_host)
    def _():
        for back in back_copies(home):
            back.wait_send()

    near = dbuf.at[0]
    remote(near, near, d_s, d_r, dev[1]).wait_recv()
    remote(raw, raw, raw_s, raw_r, dev[2]).wait_recv()
    for c, cut in enumerate(cuts):
        total = pbuf[slot[0], :, cut].astype(jnp.float32) + dbuf[0, :, cut].astype(jnp.float32)
        if c == 0:
            total = total + raw[0].astype(jnp.float32) + raw[1].astype(jnp.float32)
        else:
            x_copy(c).wait_recv()
            total = total + xr[:, cut].astype(jnp.float32)
        upd[:, cut] = (mod[2:3, cut] * total).astype(jnp.bfloat16)
    remote(near, near, d_s, d_r, dev[1]).wait_send()
    remote(raw, raw, raw_s, raw_r, dev[2]).wait_send()
    rest = pl.ds(cuts[1].start, width - cuts[1].start)
    remote(dbuf.at[1, :, rest], dbuf.at[1, :, rest], e_s, e_r.at[0], dev[1]).wait_send()
    remote(xs.at[:, rest], xs.at[:, rest], x_s, x_r.at[0], dev[2]).wait_send()


def store_kernel(upd, cache, upd_out, cache_out, sems):
    first = pltpu.make_async_copy(upd, upd_out, sems.at[0])
    second = pltpu.make_async_copy(cache, cache_out, sems.at[1])
    first.start()
    second.start()
    first.wait()
    second.wait()


def fused_device(
    patches, tokens, modulation, in_weight, query_gain, key_gain, out_weight, stale_cache, lengths
):
    rows, width = tokens.shape
    heads, head_dim = out_weight.shape[:2]
    group = 4
    all_heads = stale_cache.shape[1]
    patch_tok = rows * group
    bf, f32 = jnp.bfloat16, jnp.float32
    raw_cols = OUT_SPLIT[0] * (width // sum(OUT_SPLIT))
    later = len(OUT_SPLIT) - 1
    vm = pl.BlockSpec(memory_space=pltpu.VMEM)
    dma = pltpu.SemaphoreType.DMA
    upd, cache = pl.pallas_call(
        functools.partial(fused_kernel, patches=patches),
        out_shape=(
            jax.ShapeDtypeStruct((rows, width), bf),
            jax.ShapeDtypeStruct((rows, all_heads, 2 * head_dim), bf),
        ),
        in_specs=[pl.BlockSpec(memory_space=pltpu.HBM)] * 8,
        out_specs=(vm, vm),
        scratch_shapes=[
            pltpu.VMEM(tokens.shape, bf),
            pltpu.VMEM(modulation.shape, f32),
            pltpu.VMEM((1, head_dim), f32),
            pltpu.VMEM((1, head_dim), f32),
            pltpu.SMEM(lengths.shape, jnp.int32),
            pltpu.VMEM(stale_cache.shape, bf),
            pltpu.VMEM(in_weight.shape, bf),
            pltpu.VMEM((width, heads * 3 * head_dim), bf),
            pltpu.VMEM(out_weight.shape, bf),
            pltpu.VMEM((all_heads, rows, 2 * head_dim), bf),
            pltpu.VMEM((group, rows, width), bf),
            pltpu.VMEM((patch_tok, heads * 3 * head_dim), f32),
            pltpu.VMEM((patches, group, heads, rows, 2 * head_dim), bf),
            pltpu.VMEM((group, heads, rows, 2 * head_dim), bf),
            pltpu.VMEM((group, heads, rows, 2 * head_dim), bf),
            pltpu.VMEM((heads, patch_tok, head_dim), bf),
            pltpu.VMEM((heads, patch_tok, 1), f32),
            pltpu.VMEM((heads, patch_tok, 1), f32),
            pltpu.VMEM((heads, patch_tok, head_dim), f32),
            pltpu.VMEM((patch_tok, heads * head_dim), bf),
            pltpu.VMEM((group, rows, width), bf),
            pltpu.VMEM((2, rows, width), bf),
            pltpu.VMEM((2, rows, raw_cols), bf),
            pltpu.VMEM((rows, width), bf),
            pltpu.VMEM((rows, width), bf),
            pltpu.VMEM((SHIP, patch_tok, head_dim), bf),
            pltpu.VMEM((SHIP, patch_tok, head_dim), bf),
            pltpu.VMEM((SHIP, 8, patch_tok), f32),
            pltpu.VMEM((SHIP, patch_tok, head_dim), bf),
            pltpu.VMEM((SHIP, 8, patch_tok), f32),
            dma((6,)), dma((K_CHUNKS,)), dma, dma, dma((3,)),
            dma((patches,)), dma((patches,)), dma((patches - 1, 5)),
            dma, dma, dma, dma, dma((K_CHUNKS,)), dma((K_CHUNKS,)), dma, dma,
            dma, dma, dma, dma((later,)), dma, dma, dma, dma((later,)),
            dma, dma, dma, dma, dma, dma, dma,
        ],
        compiler_params=pltpu.CompilerParams(
            collective_id=0, has_side_effects=True, vmem_limit_bytes=48 * 1024 * 1024
        ),
    )(
        *[
            pltpu.with_memory_space_constraint(operand, pltpu.HBM)
            for operand in (
                tokens, modulation, query_gain.reshape(1, -1), key_gain.reshape(1, -1), lengths,
                stale_cache, in_weight, out_weight,
            )
        ]
    )
    return pl.pallas_call(
        store_kernel,
        out_shape=(
            jax.ShapeDtypeStruct(upd.shape, upd.dtype),
            jax.ShapeDtypeStruct(cache.shape, cache.dtype),
        ),
        in_specs=[vm, vm],
        out_specs=[pl.BlockSpec(memory_space=pltpu.HBM)] * 2,
        scratch_shapes=[dma((2,))],
        compiler_params=pltpu.CompilerParams(vmem_limit_bytes=4 * 1024 * 1024),
    )(upd, cache)


def choose(
    patches, group_shape, tokens, modulation, in_weight, query_gain, key_gain, out_weight,
    stale_cache, lengths,
):
    rows, width = tokens.shape
    heads, head_dim = out_weight.shape[:2]
    kv_bytes = patches * 4 * heads * rows * 4 * head_dim
    weight_bytes = 2 * (in_weight.size + out_weight.size)
    fits = (
        group_shape == (2, 2)
        and rows % 16 == 0
        and head_dim % 128 == 0
        and width % (128 * K_CHUNKS) == 0
        and width % (128 * sum(OUT_SPLIT)) == 0
        and width % (TURN * K_CHUNKS) == 0
        and patches == 4
        and heads > SHIP
        and rows * 4 == head_dim
        and rows * 4 * patches <= 1024
        and kv_bytes + weight_bytes <= 24 * 1024 * 1024
    )
    args = (
        tokens, modulation, in_weight, query_gain, key_gain, out_weight, stale_cache, lengths
    )
    return fused_device(patches, *args) if fits else per_device(*args)


def solution(mesh):
    return jax.shard_map(
        functools.partial(
            choose, mesh.shape["patch"], (mesh.shape["head"], mesh.shape["rep"])
        ),
        mesh=mesh,
        in_specs=(
            P(("clip", "patch", "head", "rep"), None),
            P(),
            P(None, ("head", "rep"), None),
            P(),
            P(),
            P(("head", "rep"), None, None),
            P(("clip", "patch", "head", "rep"), None, None),
            P("clip"),
        ),
        out_specs=(
            P(("clip", "patch", "head", "rep"), None),
            P(("clip", "patch", "head", "rep"), None, None),
        ),
        check_vma=False,
    )
```
